32 devices in a mesh: xy: 2 (over core), gz: 4 (over y, x), ta: 4 (over z).
Axes of the slice: x: 2, y: 2, z: 4, core: 2. Of those that a mesh axis runs over, the one named last changes fastest.
Arguments:
- right_side: float32 [2, 4, 4, 128, 128], P('xy', 'gz', 'ta'), may hold values from -40 to 40
- link_blocks: float32 [2, 4, 4, 9, 2, 32, 32, 128], P('xy', 'gz', 'ta'), may hold values from -0.75 to 0.75
Outputs:
- solution: float32 [2, 4, 4, 128, 128], P('xy', 'gz', 'ta')
- residual: float32 [2, 4, 4, 128, 128], P('xy', 'gz', 'ta')
The draws below stay inside these ranges and needn't reach their ends.
All inputs are finite; a program needn't handle non-finite values.
Results may differ from the reference program's by a relative error of at most 0.00018.
Values sent between devices are 32-bit elements; how exact they have to be, the bound alone decides.
A program may use at most 128 MiB of HBM per device.

```python
import jax
import jax.numpy as jnp
from jax import lax

DOF = 32
RHS = 2
CX = 1
NY = 8
CZ = 2
CT = 8
ITERS = 2
S = 128
VEC = 128
NT = 32
N_XY = 2
N_GZ = 4
N_TA = 4


def draw_right_side(key, part):
    noise_key, rough_key = jax.random.split(jax.random.fold_in(key, 11), 2)
    shape = (N_XY, N_GZ, N_TA, S, VEC)
    time_index = (jnp.arange(N_TA)[:, None] * CT + jnp.arange(S)[None, :] % CT).astype(jnp.float32)
    ramp = jnp.exp(jnp.log(3.0) * time_index / max(NT - 1, 1))
    ramp = ramp[None, None, :, :, None]
    rough = jnp.exp(jax.random.uniform(rough_key, (N_XY, N_GZ, N_TA, S, 1), jnp.float32, -0.8, 0.8))
    base = jax.random.normal(noise_key, shape, jnp.float32)
    return jnp.clip(base * ramp * rough, -40.0, 40.0).astype(jnp.float32)


def steps_of(stream_key, dims, cuts, smallest, largest):
    gain = 1.0
    for position, shards_of in cuts:
        steps = jax.random.uniform(jax.random.fold_in(jax.random.fold_in(stream_key, 6), position), (shards_of,), jnp.float32, smallest / len(cuts), largest / len(cuts))
        gain = gain * jnp.repeat(jnp.exp(steps), dims[position] // shards_of).reshape((-1,) + (1,) * (len(dims) - 1 - position))
    return gain


def gaussian(stream_key, dims, spread, reach, shards=(), held_as=jnp.bfloat16):
    factor_of = steps_of(stream_key, dims, shards, -0.22, 0.18) if shards else 1.0
    drawn = jax.random.normal(stream_key, dims, jnp.float32) * spread * factor_of
    return jnp.minimum(jnp.maximum(drawn, -reach), reach).astype(held_as)


def setup_inputs(seed: int = 0) -> dict:
    arg_keys = jax.random.split(jax.random.key(seed), 3)
    right_side = draw_right_side(jax.random.fold_in(arg_keys[2], 71), 0)
    link_blocks = gaussian(arg_keys[1], (N_XY, N_GZ, N_TA, 9, 2, DOF, DOF, S), (2 * DOF) ** -0.5, 0.75, ((0, 2), (1, 4), (2, 4)), jnp.float32)
    return dict(right_side=right_side, link_blocks=link_blocks)


mass_shift = 4.0
epsilon = 1e-06

def split_parts(joined):
    shaped = joined.reshape(joined.shape[:-1] + (RHS, 2, DOF))
    return (shaped[..., 0, :], shaped[..., 1, :])

def join_parts(real, imaginary):
    stacked = jnp.stack((real, imaginary), -2)
    return stacked.reshape(stacked.shape[:-3] + (-1,))

def column_sums(values):
    folded = lax.optimization_barrier(jnp.sum(values, axis=-1))
    return lax.optimization_barrier(jnp.sum(folded.reshape(-1, folded.shape[-1]), axis=0))

def to_lattice(joined):
    shaped = joined.reshape(N_XY, N_GZ, N_TA, CX, NY, CZ, CT, joined.shape[-1])
    moved = jnp.transpose(shaped, (0, 3, 4, 1, 5, 2, 6, 7))
    return moved.reshape(N_XY * CX, NY, N_GZ * CZ, N_TA * CT, joined.shape[-1])

def to_blocks(lattice):
    shaped = lattice.reshape(N_XY, CX, NY, N_GZ, CZ, N_TA, CT, lattice.shape[-1])
    moved = jnp.transpose(shaped, (0, 3, 5, 1, 2, 4, 6, 7))
    return moved.reshape(N_XY, N_GZ, N_TA, CX * NY * CZ * CT, lattice.shape[-1])

def single(blocks, field):
    return jnp.einsum('...cds,...srd->...src', blocks, field, precision=lax.Precision.HIGHEST)

def apply_operator(link_blocks, real, imaginary):
    lattice = to_lattice(join_parts(real, imaginary))
    shifted_operator = [lattice]
    for axis_number in range(4):
        shifted_operator.append(jnp.roll(lattice, -1, axis_number))
        shifted_operator.append(jnp.roll(lattice, 1, axis_number))
    out_real = mass_shift * real
    output_imaginary = mass_shift * imaginary
    for level in range(9):
        near_real, near_imag = split_parts(to_blocks(shifted_operator[level]))
        blocks_real = link_blocks[:, :, :, level, 0]
        blocks_imag = link_blocks[:, :, :, level, 1]
        out_real = out_real + single(blocks_real, near_real) - single(blocks_imag, near_imag)
        output_imaginary = output_imaginary + single(blocks_real, near_imag) + single(blocks_imag, near_real)
    return (out_real, output_imaginary)

def solve_positive_definite(matrix, target):
    size = matrix.shape[0]
    lower = {}
    for row in range(size):
        for col in range(row + 1):
            value = matrix[row, col]
            for inner in range(col):
                value = value - lower[row, inner] * lower[col, inner]
            if row == col:
                lower[row, row] = jnp.sqrt(value)
            else:
                lower[row, col] = value / lower[col, col]
    forward = []
    for row in range(size):
        value = target[row]
        for inner in range(row):
            value = value - lower[row, inner] * forward[inner]
        forward.append(value / lower[row, row])
    answer = [None] * size
    for row in reversed(range(size)):
        value = forward[row]
        for inner in range(row + 1, size):
            value = value - lower[inner, row] * answer[inner]
        answer[row] = value / lower[row, row]
    return jnp.stack(answer)

def least_squares(hessenberg_real, hessenberg_imaginary, beta):
    exact_answer_vector = lax.Precision.HIGHEST
    gram_matrix_real = jnp.einsum('sxm,szm->xzm', hessenberg_real, hessenberg_real, precision=exact_answer_vector) + jnp.einsum('sxm,szm->xzm', hessenberg_imaginary, hessenberg_imaginary, precision=exact_answer_vector)
    gram_matrix_imaginary = jnp.einsum('sxm,szm->xzm', hessenberg_real, hessenberg_imaginary, precision=exact_answer_vector) - jnp.einsum('sxm,szm->xzm', hessenberg_imaginary, hessenberg_real, precision=exact_answer_vector)
    upper = jnp.concatenate((gram_matrix_real, -gram_matrix_imaginary), 1)
    bottom = jnp.concatenate((gram_matrix_imaginary, gram_matrix_real), 1)
    system = jnp.concatenate((upper, bottom), 0)
    target = jnp.concatenate((beta[None, :] * hessenberg_real[0], -beta[None, :] * hessenberg_imaginary[0]), 0)
    answer = solve_positive_definite(system, target)
    return (answer[:ITERS], answer[ITERS:])

def reference(right_side, link_blocks):
    rhs_real, rhs_imag = split_parts(right_side)
    beta = jnp.sqrt(column_sums(rhs_real * rhs_real + rhs_imag * rhs_imag) + epsilon)
    basis = [(rhs_real / beta[:, None], rhs_imag / beta[:, None])]
    hessenberg_real = jnp.zeros((ITERS + 1, ITERS, RHS), jnp.float32)
    hessenberg_imaginary = jnp.zeros((ITERS + 1, ITERS, RHS), jnp.float32)
    for step in range(ITERS):
        work_real, work_imag = apply_operator(link_blocks, basis[step][0], basis[step][1])
        proj_real = jnp.stack([column_sums(vector[0] * work_real + vector[1] * work_imag) for vector in basis])
        proj_imag = jnp.stack([column_sums(vector[0] * work_imag - vector[1] * work_real) for vector in basis])
        for index in range(len(basis)):
            coef_real = proj_real[index][:, None]
            coef_imag = proj_imag[index][:, None]
            vector = basis[index]
            work_real = work_real - (coef_real * vector[0] - coef_imag * vector[1])
            work_imag = work_imag - (coef_real * vector[1] + coef_imag * vector[0])
        norm = jnp.sqrt(column_sums(work_real * work_real + work_imag * work_imag) + epsilon)
        hessenberg_real = hessenberg_real.at[:step + 1, step].set(proj_real)
        hessenberg_imaginary = hessenberg_imaginary.at[:step + 1, step].set(proj_imag)
        hessenberg_real = hessenberg_real.at[step + 1, step].set(norm)
        basis.append((work_real / norm[:, None], work_imag / norm[:, None]))
    coef_real, coef_imag = least_squares(hessenberg_real, hessenberg_imaginary, beta)
    sol_real = jnp.zeros_like(rhs_real)
    sol_imag = jnp.zeros_like(rhs_imag)
    for index in range(ITERS):
        weight_real = coef_real[index][:, None]
        weight_imag = coef_imag[index][:, None]
        sol_real = sol_real + weight_real * basis[index][0] - weight_imag * basis[index][1]
        sol_imag = sol_imag + weight_real * basis[index][1] + weight_imag * basis[index][0]
    image_real, image_imag = apply_operator(link_blocks, sol_real, sol_imag)
    return (join_parts(sol_real, sol_imag), join_parts(rhs_real - image_real, rhs_imag - image_imag))
```

```python
import functools

import jax
import jax.numpy as jnp
from jax import lax
from jax.experimental import pallas as pl
from jax.experimental.pallas import tpu as pltpu
from jax.sharding import PartitionSpec as P

DOF = 32
RHS = 2
NY = 8
CZ = 2
CT = 8
S = 128
E = 128
MESH = pl.DeviceIdType.MESH

mass_shift = 4.0
epsilon = 1e-06


def cmul(a, b):
    return (a[0] * b[0] - a[1] * b[1], a[0] * b[1] + a[1] * b[0])


def conj(a):
    return (a[0], -a[1])


def cadd(a, b):
    return (a[0] + b[0], a[1] + b[1])


def csub(a, b):
    return (a[0] - b[0], a[1] - b[1])


def scale(a, x):
    return (a[0] * x, a[1] * x)


def size2(a):
    return a[0] * a[0] + a[1] * a[1]


def coefficients(g00, g11, g22, g01, g02, g12):
    beta2 = g00 + epsilon
    beta = jnp.sqrt(beta2)
    inv_beta2 = 1.0 / beta2
    h00 = scale((mass_shift * g00 + g01[0], g01[1]), inv_beta2)
    a = (mass_shift - h00[0], -h00[1])
    left = g11 + size2(a) * g00 + 2.0 * cmul(conj(a), g01)[0]
    h10_2 = jnp.maximum(left, 0.0) * inv_beta2 + epsilon
    h10 = jnp.sqrt(h10_2)
    a4 = (a[0] + mass_shift, a[1])
    a_4 = scale(a, mass_shift)
    top = cadd(cadd(g02, cmul(a4, g01)), scale(a_4, g00))
    h01 = scale(top, inv_beta2 / h10)
    low = cadd(cadd(g12, scale(a4, g11)), cmul(a_4, conj(g01)))
    h11 = scale(cadd(low, cmul(conj(a), top)), inv_beta2 / h10_2)
    p = csub(a4, h11)
    q = csub(csub(a_4, scale(h01, h10)), cmul(h11, a))
    left = g22 + size2(p) * g11 + size2(q) * g00
    left = left + 2.0 * (
        cmul(p, conj(g12))[0] + cmul(q, conj(g02))[0] + cmul(cmul(conj(q), p), g01)[0]
    )
    h21_2 = jnp.maximum(left, 0.0) * (inv_beta2 / h10_2) + epsilon
    m00 = size2(h00) + h10_2
    m01 = cadd(cmul(conj(h00), h01), scale(h11, h10))
    m11 = size2(h01) + size2(h11) + h21_2
    t0 = scale(conj(h00), beta)
    t1 = scale(conj(h01), beta)
    inv_l0 = 1.0 / jnp.sqrt(m00)
    l10 = scale(conj(m01), inv_l0)
    f0 = scale(t0, inv_l0)
    inv_d = 1.0 / (m11 - size2(l10))
    y1 = scale(csub(t1, cmul(l10, f0)), inv_d)
    y0 = scale(csub(f0, cmul(conj(l10), y1)), inv_l0)
    inv_beta = 1.0 / beta
    wb = scale(y1, inv_beta / h10)
    wa = cadd(scale(y0, inv_beta), cmul(wb, a))
    return wa, wb


def kernel(
    sizes, b_hbm, l_hbm, sol_ref, res_ref,
    links, field, xbuf, zbuf, tface, tbuf, turned, acc, red,
    b_sem, l_sem, send_sem, recv_sem, sum_send, sum_recv, seen_z, seen_x,
):
    nx, nz, nt = sizes
    total_count = nx * nz * nt
    ix, iz, it = lax.axis_index("xy"), lax.axis_index("gz"), lax.axis_index("ta")
    here = (ix * nz + iz) * nt + it

    def step(axis_value, by, count):
        return lax.rem(axis_value + (by + count), count)

    def mate(delta):
        other = lax.rem(here + delta, total_count)
        plane = other // nt
        return (plane // nz, lax.rem(plane, nz), lax.rem(other, nt))

    order = [0, 3, 4, 1, 2, 7, 8, 5, 6]
    b_copy = pltpu.make_async_copy(b_hbm.at[0, 0, 0], field.at[0], b_sem)
    b_copy.start()
    l_copies = {}
    for k in order:
        l_copies[k] = pltpu.make_async_copy(l_hbm.at[0, 0, 0, k], links.at[k], l_sem.at[k])
        l_copies[k].start()

    line_x = [(step(ix, d, nx), iz, it) for d in range(1, nx)]
    line_z = [(ix, step(iz, d, nz), it) for d in range(1, nz)]
    line_t = [(ix, iz, step(it, d, nt)) for d in range(1, nt)]

    def tell(sem, devices):
        for device in devices:
            pl.semaphore_signal(sem, inc=1, device_id=device, device_id_type=MESH)

    barrier = pltpu.get_barrier_semaphore()
    tell(barrier, line_t + line_z + line_x)
    pl.semaphore_wait(barrier, len(line_t) + len(line_z) + len(line_x))
    tell(seen_z, line_z)
    b_copy.wait()

    lane = lax.broadcasted_iota(jnp.int32, (S, E), 1)
    in_t = lane % CT
    in_z = (lane // CT) % CZ
    row8 = lax.broadcasted_iota(jnp.int32, (8, 128), 0)

    def halo(n):
        mine = field.at[n]
        tface[n, 0] = field[n, pl.ds(0, NY * CZ, stride=CT), :]
        tface[n, 1] = field[n, pl.ds(CT - 1, NY * CZ, stride=CT), :]
        tiles = mine.reshape(NY, CZ, CT, E)
        moves = []
        for way in (0, 1):
            by = 1 if way else -1
            moves.append(("t%d" % way, tface.at[n, way], tbuf.at[n, way], (ix, iz, step(it, by, nt))))
        for way in (0, 1):
            by = 1 if way else -1
            moves.append(
                ("z%d" % way, tiles.at[:, way * (CZ - 1)], zbuf.at[n].reshape(NY, CZ, CT, E).at[:, (1 - way) * (CZ - 1)],
                 (ix, step(iz, by, nz), it))
            )
        for way in (0, 1) if nx > 2 else (0,):
            by = 1 if way else -1
            moves.append(("x%d" % way, mine, xbuf.at[n, way], (step(ix, by, nx), iz, it)))
        copies = {}
        for number, (name, source, target, device) in enumerate(moves):
            copy = pltpu.make_async_remote_copy(
                src_ref=source, dst_ref=target,
                send_sem=send_sem.at[n, number], recv_sem=recv_sem.at[n, number],
                device_id=device, device_id_type=MESH,
            )
            copy.start()
            copies[name] = copy
        return copies

    def products(passes, fresh, merge=False):
        def body(c, carry):
            if fresh:
                sums = [jnp.zeros((8, 128), jnp.float32) for _ in range(4)]
            else:
                sums = [acc[i, c] for i in range(4)]
            for link, near in passes:
                for j in range(DOF // 8):
                    rows = pl.ds(8 * j, 8)
                    lr = links[link, 0, c, rows, :]
                    li = links[link, 1, c, rows, :]
                    if merge:
                        lr = lr + links[link + 1, 0, c, rows, :]
                        li = li + links[link + 1, 1, c, rows, :]
                        links[link, 0, c, rows, :] = lr
                        links[link, 1, c, rows, :] = li
                    for r in range(RHS):
                        vr = turned[near, pl.ds(2 * r * DOF + 8 * j, 8), :]
                        vi = turned[near, pl.ds((2 * r + 1) * DOF + 8 * j, 8), :]
                        sums[2 * r] = sums[2 * r] + lr * vr - li * vi
                        sums[2 * r + 1] = sums[2 * r + 1] + lr * vi + li * vr
            for i in range(4):
                acc[i, c] = sums[i]
            return carry

        lax.fori_loop(0, DOF, body, 0, unroll=2)

    lane8 = lax.broadcasted_iota(jnp.int32, (8, 128), 1)

    def split_links():
        inner = (lane8 // CT) % CZ == 0
        last = lane8 % CT == CT - 1

        def body(c, carry):
            for p in range(2):
                for j in range(DOF // 8):
                    rows = pl.ds(8 * j, 8)
                    up, down = links[5, p, c, rows, :], links[6, p, c, rows, :]
                    links[5, p, c, rows, :] = jnp.where(inner, up, down)
                    links[6, p, c, rows, :] = jnp.where(inner, down, up)
                    up, down = links[7, p, c, rows, :], links[8, p, c, rows, :]
                    links[9, p, c, rows, :] = jnp.where(last, up, down)
            return carry

        lax.fori_loop(0, DOF, body, 0, unroll=2)

    def fold(xs):
        low = row8 < 4
        ys = [
            jnp.where(low, xs[i], xs[i + 4]) + pltpu.roll(jnp.where(low, xs[i + 4], xs[i]), 4, 0)
            for i in range(4)
        ]
        low = row8 % 4 < 2
        zs = [
            jnp.where(low, ys[i] + pltpu.roll(ys[i], 6, 0), ys[i + 2] + pltpu.roll(ys[i + 2], 2, 0))
            for i in range(2)
        ]
        return jnp.where(
            row8 % 2 < 1, zs[0] + pltpu.roll(zs[0], 7, 0), zs[1] + pltpu.roll(zs[1], 1, 0)
        )

    def apply(n, copies):
        own = turned[0]
        turned[3] = pltpu.roll(own, S - CZ * CT, 1)
        turned[4] = pltpu.roll(own, CZ * CT, 1)
        turned[5] = jnp.where(in_z == 0, pltpu.roll(own, S - CT, 1), pltpu.roll(own, CT, 1))
        turned[7] = jnp.where(in_t == CT - 1, 0.0, pltpu.roll(own, S - 1, 1))
        turned[8] = jnp.where(in_t == 0, 0.0, pltpu.roll(own, 1, 1))
        if n == 0:
            for k in range(9):
                l_copies[k].wait()
            split_links()
        products(((0, 0), (3, 3), (4, 4)), True)
        products(((5, 5), (7, 7), (8, 8)), False)
        copies["x0"].wait_recv()
        turned[1] = xbuf[n, 0].T
        if nx > 2:
            copies["x1"].wait_recv()
            turned[2] = xbuf[n, 1].T
            products(((1, 1), (2, 2)), False)
        else:
            products(((1, 1),), False, n == 0)
        copies["z0"].wait_recv()
        copies["z1"].wait_recv()
        turned[6] = zbuf[n].T
        products(((6, 6),), False)
        copies["t0"].wait_recv()
        copies["t1"].wait_recv()
        edge = field.at[3]
        edge[pl.ds(CT - 1, NY * CZ, stride=CT), :] = tbuf[n, 0]
        edge[pl.ds(0, NY * CZ, stride=CT), :] = tbuf[n, 1]
        turned[9] = edge[...].T
        products(((9, 9),), False)
        for i in range(4):
            for c in range(0, DOF, 8):
                turned[0, pl.ds(i * DOF + c, 8), :] = fold([acc[i, c + j] for j in range(8)])
        field[n + 1] = turned[0].T

    field[3] = jnp.zeros((S, E), jnp.float32)
    first = halo(0)
    pl.semaphore_wait(seen_z, len(line_z))
    tell(seen_x, line_x)
    turned[0] = field[0].T
    apply(0, first)
    second = halo(1)
    apply(1, second)

    in_p = (lax.broadcasted_iota(jnp.int32, (S, E), 1) // DOF) % 2

    def aside(v):
        return jnp.where(in_p == 0, pltpu.roll(v, E - DOF, 1), -pltpu.roll(v, DOF, 1))

    def total(u, v):
        return jnp.sum((u * v).reshape(S // 8, 8, E), axis=0)

    pl.semaphore_wait(seen_x, len(line_x))
    k0, k1, k2 = field[0], field[1], field[2]
    z1, z2 = aside(k1), aside(k2)
    sums = [
        total(k0, k0), total(k1, k1), total(k2, k2), total(k0, k1), total(k0, z1),
        total(k0, k2), total(k0, z2),
    ]
    first_p = in_p[:8] == 0

    def both(v):
        return v + jnp.where(first_p, pltpu.roll(v, E - DOF, 1), pltpu.roll(v, DOF, 1))

    sums.append(jnp.where(first_p, both(total(k1, k2)), both(total(k1, z2))))
    lanes = fold(sums)
    for width in (16, 8, 4):
        low = lane8 % (2 * width) < width
        lanes = lanes + jnp.where(
            low, pltpu.roll(lanes, 128 - width, 1), pltpu.roll(lanes, width, 1)
        )
    seat = (lane8 % DOF) // 4 == row8
    red[0] = jnp.sum(jnp.where(seat, lanes, 0.0), axis=0, keepdims=True)
    sent = []
    for delta in range(1, total_count):
        copy = pltpu.make_async_remote_copy(
            src_ref=red.at[0], dst_ref=red.at[delta],
            send_sem=sum_send.at[delta], recv_sem=sum_recv.at[delta],
            device_id=mate(delta), device_id_type=MESH,
        )
        copy.start()
        sent.append(copy)
    for copy in sent:
        copy.wait_recv()
    value = jnp.where(seat, jnp.sum(red[...], axis=0), 0.0)
    quarter = lax.broadcasted_iota(jnp.int32, (8, 128), 1) // DOF
    sum00, sum01, sum10, sum11 = [
        jnp.sum(jnp.where(quarter == i, value, 0.0), axis=1, keepdims=True) for i in range(4)
    ]
    half = quarter < 2
    gram = jnp.where(half, sum00 + sum01, sum10 + sum11)
    g = [gram[i : i + 1] for i in range(7)]
    g.append(jnp.where(half, sum00, sum10)[7:8])
    g.append(jnp.where(half, sum01, sum11)[7:8])
    wa, wb = coefficients(g[0], g[1], g[2], (g[3], g[4]), (g[5], g[6]), (g[7], g[8]))

    def weighted(w, v, z):
        return w[0] * v - w[1] * z

    k0, k1, k2 = field[0], field[1], field[2]
    z0, z1, z2 = aside(k0), aside(k1), aside(k2)
    sol = weighted(wa, k0, z0) + weighted(wb, k1, z1)
    image = weighted(wa, k1, z1) + weighted(wb, k2, z2)
    sol_ref[0, 0, 0] = sol
    res_ref[0, 0, 0] = k0 - mass_shift * sol - image
    for copies in (first, second):
        for copy in copies.values():
            copy.wait_send()
    for copy in sent:
        copy.wait_send()


def deliver(a_ref, b_ref, sol_ref, res_ref):
    sol_ref[...] = a_ref[...]
    res_ref[...] = b_ref[...]


def shards(sizes, right_side, link_blocks):
    nx, nz, nt = sizes
    out = jax.ShapeDtypeStruct(right_side.shape, jnp.float32)
    f32 = jnp.float32
    moves = 6 if nx > 2 else 5
    held = pltpu.VMEM(right_side.shape, f32)
    results = pl.pallas_call(
        functools.partial(kernel, sizes),
        out_shape=(held, held),
        in_specs=[pl.BlockSpec(memory_space=pl.ANY)] * 2,
        out_specs=(pl.BlockSpec(memory_space=pltpu.VMEM),) * 2,
        scratch_shapes=[
            pltpu.VMEM((10, 2, DOF, DOF, S), f32),
            pltpu.VMEM((4, S, E), f32),
            pltpu.VMEM((2, 2, S, E), f32),
            pltpu.VMEM((2, S, E), f32),
            pltpu.VMEM((2, 2, NY * CZ, E), f32),
            pltpu.VMEM((2, 2, NY * CZ, E), f32),
            pltpu.VMEM((10, E, S), f32),
            pltpu.VMEM((4, DOF, 8, S), f32),
            pltpu.VMEM((nx * nz * nt, 1, 128), f32),
            pltpu.SemaphoreType.DMA,
            pltpu.SemaphoreType.DMA((9,)),
            pltpu.SemaphoreType.DMA((2, moves)),
            pltpu.SemaphoreType.DMA((2, moves)),
            pltpu.SemaphoreType.DMA((nx * nz * nt,)),
            pltpu.SemaphoreType.DMA((nx * nz * nt,)),
            pltpu.SemaphoreType.REGULAR,
            pltpu.SemaphoreType.REGULAR,
        ],
        compiler_params=pltpu.CompilerParams(
            collective_id=0, has_side_effects=True, vmem_limit_bytes=56 * 1024 * 1024
        ),
    )(right_side, link_blocks)
    return pl.pallas_call(
        deliver,
        out_shape=(out, out),
        in_specs=[pl.BlockSpec(memory_space=pltpu.VMEM)] * 2,
        out_specs=(pl.BlockSpec(memory_space=pltpu.VMEM),) * 2,
    )(*[pltpu.with_memory_space_constraint(x, pltpu.VMEM) for x in results])


def solution(mesh):
    sizes = tuple(mesh.shape[name] for name in ("xy", "gz", "ta"))
    return jax.shard_map(
        functools.partial(shards, sizes),
        mesh=mesh,
        in_specs=(
            P("xy", "gz", "ta", None, None),
            P("xy", "gz", "ta", None, None, None, None, None),
        ),
        out_specs=(P("xy", "gz", "ta", None, None), P("xy", "gz", "ta", None, None)),
        check_vma=False,
    )
```

```python
import functools

import jax
import jax.numpy as jnp
from jax import lax
from jax.experimental import pallas as pl
from jax.experimental.pallas import tpu as pltpu
from jax.sharding import PartitionSpec as P

DOF = 32
RHS = 2
NY = 8
CZ = 2
CT = 8
S = 128
E = 128
MESH = pl.DeviceIdType.MESH

mass_shift = 4.0
epsilon = 1e-06


def cmul(a, b):
    return (a[0] * b[0] - a[1] * b[1], a[0] * b[1] + a[1] * b[0])


def conj(a):
    return (a[0], -a[1])


def cadd(a, b):
    return (a[0] + b[0], a[1] + b[1])


def csub(a, b):
    return (a[0] - b[0], a[1] - b[1])


def scale(a, x):
    return (a[0] * x, a[1] * x)


def size2(a):
    return a[0] * a[0] + a[1] * a[1]


def coefficients(g00, g11, g22, g01, g02, g12):
    beta2 = g00 + epsilon
    beta = jnp.sqrt(beta2)
    inv_beta2 = 1.0 / beta2
    h00 = scale((mass_shift * g00 + g01[0], g01[1]), inv_beta2)
    a = (mass_shift - h00[0], -h00[1])
    left = g11 + size2(a) * g00 + 2.0 * cmul(conj(a), g01)[0]
    h10_2 = jnp.maximum(left, 0.0) * inv_beta2 + epsilon
    h10 = jnp.sqrt(h10_2)
    a4 = (a[0] + mass_shift, a[1])
    a_4 = scale(a, mass_shift)
    top = cadd(cadd(g02, cmul(a4, g01)), scale(a_4, g00))
    h01 = scale(top, inv_beta2 / h10)
    low = cadd(cadd(g12, scale(a4, g11)), cmul(a_4, conj(g01)))
    h11 = scale(cadd(low, cmul(conj(a), top)), inv_beta2 / h10_2)
    p = csub(a4, h11)
    q = csub(csub(a_4, scale(h01, h10)), cmul(h11, a))
    left = g22 + size2(p) * g11 + size2(q) * g00
    left = left + 2.0 * (
        cmul(p, conj(g12))[0] + cmul(q, conj(g02))[0] + cmul(cmul(conj(q), p), g01)[0]
    )
    h21_2 = jnp.maximum(left, 0.0) * (inv_beta2 / h10_2) + epsilon
    m00 = size2(h00) + h10_2
    m01 = cadd(cmul(conj(h00), h01), scale(h11, h10))
    m11 = size2(h01) + size2(h11) + h21_2
    t0 = scale(conj(h00), beta)
    t1 = scale(conj(h01), beta)
    inv_l0 = 1.0 / jnp.sqrt(m00)
    l10 = scale(conj(m01), inv_l0)
    f0 = scale(t0, inv_l0)
    inv_d = 1.0 / (m11 - size2(l10))
    y1 = scale(csub(t1, cmul(l10, f0)), inv_d)
    y0 = scale(csub(f0, cmul(conj(l10), y1)), inv_l0)
    inv_beta = 1.0 / beta
    wb = scale(y1, inv_beta / h10)
    wa = cadd(scale(y0, inv_beta), cmul(wb, a))
    return wa, wb


def kernel(
    sizes, b_hbm, l_hbm, sol_ref, res_ref,
    links, edge_links, field, kv, turned, xbuf, zbuf, zpack, tbuf, tpack, acc, red,
    b_sem, l_sem, sent, got, got_sum, seen_z, seen_x,
):
    nx, nz, nt = sizes
    total_count = nx * nz * nt
    ix, iz, it = lax.axis_index("xy"), lax.axis_index("gz"), lax.axis_index("ta")
    here = (ix * nz + iz) * nt + it
    groups = DOF // 8
    ways = 2 if nx > 2 else 1

    def step(axis_value, by, count):
        return lax.rem(axis_value + (by + count), count)

    def at(x, z, t):
        return (x, z, t)

    line_x = [at(step(ix, d, nx), iz, it) for d in range(1, nx)]
    line_z = [at(ix, step(iz, d, nz), it) for d in range(1, nz)]
    line_t = [at(ix, iz, step(it, d, nt)) for d in range(1, nt)]

    def tell(sem, devices):
        for device in devices:
            pl.semaphore_signal(sem, inc=1, device_id=device, device_id_type=MESH)

    def remote(source, target, send_sem, recv_sem, device):
        return pltpu.make_async_remote_copy(
            src_ref=source, dst_ref=target, send_sem=send_sem, recv_sem=recv_sem,
            device_id=device, device_id_type=MESH,
        )

    barrier = pltpu.get_barrier_semaphore()
    tell(barrier, line_t + line_z + line_x)

    b_copy = pltpu.make_async_copy(b_hbm.at[0, 0, 0], field.at[0], b_sem)
    b_copy.start()
    l_copies = {}
    for number, (k, count) in enumerate(((0, 1), (3, 2), (7, 2), (5, 2), (1, 2))):
        part = pl.ds(k, count)
        l_copies[k] = pltpu.make_async_copy(l_hbm.at[0, 0, 0, part], links.at[part], l_sem.at[number])
        l_copies[k].start()

    lane = lax.broadcasted_iota(jnp.int32, (8, 128), 1)
    row8 = lax.broadcasted_iota(jnp.int32, (8, 128), 0)
    in_t = lane % CT
    in_z = (lane // CT) % CZ
    odd = lane % 2 == 1

    def rolled(x, by):
        return pltpu.roll(x, by % S, 1) if by % S else x

    def seat(j):
        return (in_t == 2 * j) | (in_t == (2 * j + CT - 1) % CT)

    seats = [seat(j) for j in range(groups)]

    def tiles(ref, first, count):
        return [ref[pl.ds(first + 8 * j, 8), :] for j in range(count)]

    def halo(n):
        mine = kv.at[n]
        for i in range(2 * RHS):
            rows = tiles(mine, i * DOF, groups)
            packed = None
            for j in range(groups):
                part = jnp.where(odd, rolled(rows[j], 2 * j + CT - 1), rolled(rows[j], 2 * j - CT + 1))
                packed = part if packed is None else jnp.where(seats[j], part, packed)
            tpack[n, pl.ds(8 * i, 8), :] = packed
        for way in (0, 1):
            by = 1 if way else -1
            remote(tpack.at[n], tbuf.at[n, way], sent.at[0], got.at[n, 0], at(ix, iz, step(it, by, nt))).start()
        half = RHS * DOF
        for j in range(half // 8):
            a = mine[pl.ds(8 * j, 8), :]
            b = mine[pl.ds(half + 8 * j, 8), :]
            zpack[n, 0, pl.ds(8 * j, 8), :] = jnp.where(in_z == 0, a, rolled(b, CT))
            zpack[n, 1, pl.ds(8 * j, 8), :] = jnp.where(in_z == 0, rolled(a, -CT), b)
        for way in (0, 1):
            by = 1 if way else -1
            remote(zpack.at[n, way], zbuf.at[n, way], sent.at[1], got.at[n, 1], at(ix, step(iz, by, nz), it)).start()
        for way in range(ways):
            by = 1 if way else -1
            remote(mine, xbuf.at[n, way], sent.at[2], got.at[n, 2], at(step(ix, by, nx), iz, it)).start()

    def receive(n, kind, ref):
        remote(ref, ref, sent.at[kind], got.at[n, kind], (ix, iz, it)).wait_recv()

    def products(passes, fresh, merge=False, final=False):
        def block(c0):
            sums = [[None] * (3 * RHS) for _ in range(4)]
            for link, near in passes:
                for j in range(groups):
                    rows = pl.ds(8 * j, 8)
                    vs = []
                    for r in range(RHS):
                        vr = near[pl.ds(2 * r * DOF + 8 * j, 8), :]
                        vi = near[pl.ds((2 * r + 1) * DOF + 8 * j, 8), :]
                        vs += [vr, vi, vr + vi]
                    for q in range(4):
                        c = c0 + q
                        lr = links[link, 0, c, rows, :]
                        li = links[link, 1, c, rows, :]
                        if merge:
                            lr = lr + links[link + 1, 0, c, rows, :]
                            li = li + links[link + 1, 1, c, rows, :]
                            links[link, 0, c, rows, :] = lr
                            links[link, 1, c, rows, :] = li
                        ls = (lr, li, lr + li)
                        for m in range(3 * RHS):
                            x = ls[m % 3] * vs[m]
                            sums[q][m] = x if sums[q][m] is None else sums[q][m] + x
            out = []
            for q in range(4):
                parts = []
                for r in range(RHS):
                    rr, ii, both = sums[q][3 * r : 3 * r + 3]
                    parts += [rr - ii, both - (rr + ii)]
                if not fresh:
                    parts = [acc[i, c0 + q] + parts[i] for i in range(2 * RHS)]
                out.append(parts)
            return out

        def body(step_number, carry):
            if final:
                c0 = step_number * 8
                out = block(c0) + block(c0 + 4)
                for i in range(2 * RHS):
                    rows = pl.ds(pl.multiple_of(i * DOF + c0, 8), 8)
                    turned[0, rows, :] = fold([out[q][i] for q in range(8)])
            else:
                c0 = step_number * 4
                out = block(c0)
                for q in range(4):
                    for i in range(2 * RHS):
                        acc[i, c0 + q] = out[q][i]
            return carry

        lax.fori_loop(0, DOF // (8 if final else 4), body, 0)

    def split_z():
        def body(c, carry):
            for p in range(2):
                for j in range(groups):
                    rows = pl.ds(8 * j, 8)
                    up, down = links[5, p, c, rows, :], links[6, p, c, rows, :]
                    links[5, p, c, rows, :] = jnp.where(in_z == 0, up, down)
                    links[6, p, c, rows, :] = jnp.where(in_z == 0, down, up)
            return carry

        lax.fori_loop(0, DOF, body, 0, unroll=2)

    def pack_edges():
        last = in_t == CT - 1

        def body(c, carry):
            for p in range(2):
                packed = None
                for j in range(groups):
                    rows = pl.ds(8 * j, 8)
                    part = rolled(jnp.where(last, links[7, p, c, rows, :], links[8, p, c, rows, :]), 2 * j)
                    packed = part if packed is None else jnp.where(seats[j], part, packed)
                edge_links[p, c] = packed
            return carry

        lax.fori_loop(0, DOF, body, 0, unroll=8)

    low4, low2, low1 = row8 < 4, row8 % 4 < 2, row8 % 2 < 1

    def fold(xs):
        ys = [
            jnp.where(low4, xs[i], xs[i + 4]) + pltpu.roll(jnp.where(low4, xs[i + 4], xs[i]), 4, 0)
            for i in range(4)
        ]
        zs = [
            jnp.where(low2, ys[i] + pltpu.roll(ys[i], 6, 0), ys[i + 2] + pltpu.roll(ys[i + 2], 2, 0))
            for i in range(2)
        ]
        return jnp.where(low1, zs[0] + pltpu.roll(zs[0], 7, 0), zs[1] + pltpu.roll(zs[1], 1, 0))

    def shift(n):
        mine = kv.at[n]
        for j in range(E // 8):
            rows = pl.ds(8 * j, 8)
            own = mine[rows, :]
            turned[0, rows, :] = rolled(own, -CZ * CT)
            turned[1, rows, :] = rolled(own, CZ * CT)
            turned[2, rows, :] = jnp.where(in_z == 0, rolled(own, -CT), rolled(own, CT))
            turned[3, rows, :] = jnp.where(in_t == CT - 1, 0.0, rolled(own, -1))
            turned[4, rows, :] = jnp.where(in_t == 0, 0.0, rolled(own, 1))

    local = ((0, None), (3, 0), (4, 1), (7, 3), (8, 4), (5, 2))

    def apply(n):
        shift(n)
        terms = [(link, kv.at[n] if near is None else turned.at[near]) for link, near in local]
        if n == 0:
            l_copies[0].wait()
            l_copies[3].wait()
            products(terms[:3], True)
            l_copies[7].wait()
            products(terms[3:5], False)
            pack_edges()
            l_copies[5].wait()
            split_z()
            products(terms[5:], False)
            pl.semaphore_wait(seen_z, len(line_z))
            tell(seen_x, line_x)
            l_copies[1].wait()
        else:
            products(terms, True)
            early()
        receive(n, 2, xbuf.at[n, pl.ds(0, ways)])
        if nx > 2:
            products(((1, xbuf.at[n, 0]), (2, xbuf.at[n, 1])), False)
        else:
            products(((1, xbuf.at[n, 0]),), False, n == 0)
        receive(n, 1, zbuf.at[n])
        half = RHS * DOF
        for j in range(half // 8):
            p0 = zbuf[n, 0, pl.ds(8 * j, 8), :]
            p1 = zbuf[n, 1, pl.ds(8 * j, 8), :]
            turned[2, pl.ds(8 * j, 8), :] = jnp.where(in_z == 0, p1, rolled(p0, CT))
            turned[2, pl.ds(half + 8 * j, 8), :] = jnp.where(in_z == 0, rolled(p1, -CT), p0)
        products(((6, turned.at[2]),), False, final=True)
        receive(n, 0, tbuf.at[n])
        vs = [
            jnp.where(odd, tbuf[n, 0, pl.ds(8 * i, 8), :], tbuf[n, 1, pl.ds(8 * i, 8), :])
            for i in range(4)
        ]
        for c in range(0, DOF, 8):
            parts = [[] for _ in range(4)]
            for j in range(8):
                lr, li = edge_links[0, c + j], edge_links[1, c + j]
                for r in range(RHS):
                    vr, vi = vs[2 * r], vs[2 * r + 1]
                    parts[2 * r].append(lr * vr - li * vi)
                    parts[2 * r + 1].append(lr * vi + li * vr)
            for i in range(4):
                d = fold(parts[i])
                d = d + rolled(d, -2)
                d = d + rolled(d, -4)
                rows = pl.ds(i * DOF + c, 8)
                kv[n + 1, rows, :] = turned[0, rows, :] + jnp.where(seats[0], d, 0.0)

    def dots(a, b, both):
        out = []
        for r in range(RHS):
            re = im = None
            for j in range(groups):
                ar, ai = (a[pl.ds((2 * r + p) * DOF + 8 * j, 8), :] for p in range(2))
                br, bi = (b[pl.ds((2 * r + p) * DOF + 8 * j, 8), :] for p in range(2))
                x = ar * br + ai * bi
                re = x if re is None else re + x
                if both:
                    x = ar * bi - ai * br
                    im = x if im is None else im + x
            out.append((re, im) if both else (re,))
        return out

    def lane_sums(x):
        return jnp.broadcast_to(jnp.sum(x, axis=1, keepdims=True), (8, 128))

    def early():
        d00, d11, d01 = dots(kv.at[0], kv.at[0], False), dots(kv.at[1], kv.at[1], False), dots(kv.at[0], kv.at[1], True)
        sums = lane_sums(fold([x for r in range(RHS) for x in d00[r] + d11[r] + d01[r]]))
        acc_row = jnp.where(lane == row8, sums, 0.0)
        field[4, pl.ds(0, 8), :] = acc_row

    b_copy.wait()
    kv[0] = field[0].T
    pl.semaphore_wait(barrier, len(line_t) + len(line_z) + len(line_x))
    halo(0)
    tell(seen_z, line_z)
    apply(0)
    halo(1)
    apply(1)

    d02, d12, d22 = dots(kv.at[0], kv.at[2], True), dots(kv.at[1], kv.at[2], True), dots(kv.at[2], kv.at[2], False)
    sums = lane_sums(fold([x for r in range(RHS) for x in d02[r] + d12[r]]))
    a, b = d22[0][0], d22[1][0]
    norms = lane_sums(jnp.where(low4, a + pltpu.roll(a, 4, 0), b + pltpu.roll(b, 4, 0)))
    mine = field[4, pl.ds(0, 8), :] + jnp.where(lane == 8 + row8, sums, 0.0)
    mine = mine + jnp.where(lane == 16 + row8 // 4, norms, 0.0)
    pl.semaphore_wait(seen_x, len(line_x))
    red[here] = jnp.sum(mine, axis=0, keepdims=True)
    for number in range(total_count - 1):
        other = number + jnp.where(here <= number, 1, 0)
        plane = lax.div(other, nt)
        device = (lax.div(plane, nz), lax.rem(plane, nz), lax.rem(other, nt))
        remote(red.at[here], red.at[here], sent.at[3], got_sum, device).start()

    in_p = (lax.broadcasted_iota(jnp.int32, (S, E), 1) // DOF) % 2

    def aside(v):
        return jnp.where(in_p == 0, pltpu.roll(v, E - DOF, 1), -pltpu.roll(v, DOF, 1))

    k1, k2 = kv[1].T, kv[2].T
    field[1] = k1
    field[2] = k2
    turned[0] = aside(field[0])
    turned[1] = aside(k1)
    turned[2] = aside(k2)
    for kind, ref in ((0, tbuf), (1, zbuf), (2, xbuf.at[:, pl.ds(0, ways)])):
        remote(ref, ref, sent.at[kind], got_sum, (ix, iz, it)).wait_send()

    others = red.at[pl.ds(0, total_count - 1)]
    remote(others, others, sent.at[3], got_sum, (ix, iz, it)).wait_recv()
    value = jnp.broadcast_to(jnp.sum(red[...], axis=0), (8, 128))
    first_half = lane < 2 * DOF

    def pick(place):
        return [jnp.sum(jnp.where(lane == place + by * r, value, 0.0), axis=1, keepdims=True) for r, by in ((0, 0), (1, 4))]

    place = (row8 // 4) * 8 + row8 % 4
    low, high = pick(place)
    gram = jnp.where(first_half, low, high)
    low, _ = pick(16 + row8 * 0)
    high, _ = pick(17 + row8 * 0)
    g22 = jnp.where(first_half, low, high)[0:1]
    g = [gram[i : i + 1] for i in range(8)]
    wa, wb = coefficients(g[0], g[1], g22, (g[2], g[3]), (g[4], g[5]), (g[6], g[7]))

    def weighted(w, v, z):
        return w[0] * v - w[1] * z

    k0, k1, k2 = field[0], field[1], field[2]
    z0, z1, z2 = turned[0], turned[1], turned[2]
    sol = weighted(wa, k0, z0) + weighted(wb, k1, z1)
    image = weighted(wa, k1, z1) + weighted(wb, k2, z2)
    sol_ref[0, 0, 0] = sol
    res_ref[0, 0, 0] = k0 - mass_shift * sol - image
    remote(others, others, sent.at[3], got_sum, (ix, iz, it)).wait_send()


def deliver(a_ref, b_ref, sol_ref, res_ref):
    sol_ref[...] = a_ref[...]
    res_ref[...] = b_ref[...]


def shards(sizes, right_side, link_blocks):
    nx, nz, nt = sizes
    out = jax.ShapeDtypeStruct(right_side.shape, jnp.float32)
    f32 = jnp.float32
    held = pltpu.VMEM(right_side.shape, f32)
    results = pl.pallas_call(
        functools.partial(kernel, sizes),
        out_shape=(held, held),
        in_specs=[pl.BlockSpec(memory_space=pl.ANY)] * 2,
        out_specs=(pl.BlockSpec(memory_space=pltpu.VMEM),) * 2,
        scratch_shapes=[
            pltpu.VMEM((9, 2, DOF, DOF, S), f32),
            pltpu.VMEM((2, DOF, 8, S), f32),
            pltpu.VMEM((5, S, E), f32),
            pltpu.VMEM((3, E, S), f32),
            pltpu.VMEM((5, E, S), f32),
            pltpu.VMEM((2, 2 if nx > 2 else 1, E, S), f32),
            pltpu.VMEM((2, 2, RHS * DOF, S), f32),
            pltpu.VMEM((2, 2, RHS * DOF, S), f32),
            pltpu.VMEM((2, 2, 2 * RHS * 8, S), f32),
            pltpu.VMEM((2, 2 * RHS * 8, S), f32),
            pltpu.VMEM((4, DOF, 8, S), f32),
            pltpu.VMEM((nx * nz * nt, 1, 128), f32),
            pltpu.SemaphoreType.DMA,
            pltpu.SemaphoreType.DMA((5,)),
            pltpu.SemaphoreType.DMA((4,)),
            pltpu.SemaphoreType.DMA((2, 3)),
            pltpu.SemaphoreType.DMA,
            pltpu.SemaphoreType.REGULAR,
            pltpu.SemaphoreType.REGULAR,
        ],
        compiler_params=pltpu.CompilerParams(
            collective_id=0, has_side_effects=True, vmem_limit_bytes=56 * 1024 * 1024
        ),
    )(right_side, link_blocks)
    return pl.pallas_call(
        deliver,
        out_shape=(out, out),
        in_specs=[pl.BlockSpec(memory_space=pltpu.VMEM)] * 2,
        out_specs=(pl.BlockSpec(memory_space=pltpu.VMEM),) * 2,
    )(*[pltpu.with_memory_space_constraint(x, pltpu.VMEM) for x in results])


def solution(mesh):
    sizes = tuple(mesh.shape[name] for name in ("xy", "gz", "ta"))
    return jax.shard_map(
        functools.partial(shards, sizes),
        mesh=mesh,
        in_specs=(
            P("xy", "gz", "ta", None, None),
            P("xy", "gz", "ta", None, None, None, None, None),
        ),
        out_specs=(P("xy", "gz", "ta", None, None), P("xy", "gz", "ta", None, None)),
        check_vma=False,
    )
```

```python
import functools
import itertools

import jax
import jax.numpy as jnp
from jax import lax
from jax.experimental import pallas as pl
from jax.experimental.pallas import tpu as pltpu
from jax.sharding import PartitionSpec as P

DOF = 32
RHS = 2
NY = 8
CZ = 2
CT = 8
S = 128
E = 128
MESH = pl.DeviceIdType.MESH

mass_shift = 4.0
epsilon = 1e-06


def cmul(a, b):
    return (a[0] * b[0] - a[1] * b[1], a[0] * b[1] + a[1] * b[0])


def conj(a):
    return (a[0], -a[1])


def cadd(a, b):
    return (a[0] + b[0], a[1] + b[1])


def csub(a, b):
    return (a[0] - b[0], a[1] - b[1])


def scale(a, x):
    return (a[0] * x, a[1] * x)


def size2(a):
    return a[0] * a[0] + a[1] * a[1]


def coefficients(g00, g11, g22, g01, g02, g12):
    beta2 = g00 + epsilon
    beta = jnp.sqrt(beta2)
    inv_beta2 = 1.0 / beta2
    h00 = scale((mass_shift * g00 + g01[0], g01[1]), inv_beta2)
    a = (mass_shift - h00[0], -h00[1])
    left = g11 + size2(a) * g00 + 2.0 * cmul(conj(a), g01)[0]
    h10_2 = jnp.maximum(left, 0.0) * inv_beta2 + epsilon
    h10 = jnp.sqrt(h10_2)
    a4 = (a[0] + mass_shift, a[1])
    a_4 = scale(a, mass_shift)
    top = cadd(cadd(g02, cmul(a4, g01)), scale(a_4, g00))
    h01 = scale(top, inv_beta2 / h10)
    low = cadd(cadd(g12, scale(a4, g11)), cmul(a_4, conj(g01)))
    h11 = scale(cadd(low, cmul(conj(a), top)), inv_beta2 / h10_2)
    p = csub(a4, h11)
    q = csub(csub(a_4, scale(h01, h10)), cmul(h11, a))
    left = g22 + size2(p) * g11 + size2(q) * g00
    left = left + 2.0 * (
        cmul(p, conj(g12))[0] + cmul(q, conj(g02))[0] + cmul(cmul(conj(q), p), g01)[0]
    )
    h21_2 = jnp.maximum(left, 0.0) * (inv_beta2 / h10_2) + epsilon
    m00 = size2(h00) + h10_2
    m01 = cadd(cmul(conj(h00), h01), scale(h11, h10))
    m11 = size2(h01) + size2(h11) + h21_2
    t0 = scale(conj(h00), beta)
    t1 = scale(conj(h01), beta)
    inv_l0 = 1.0 / jnp.sqrt(m00)
    l10 = scale(conj(m01), inv_l0)
    f0 = scale(t0, inv_l0)
    inv_d = 1.0 / (m11 - size2(l10))
    y1 = scale(csub(t1, cmul(l10, f0)), inv_d)
    y0 = scale(csub(f0, cmul(conj(l10), y1)), inv_l0)
    inv_beta = 1.0 / beta
    wb = scale(y1, inv_beta / h10)
    wa = cadd(scale(y0, inv_beta), cmul(wb, a))
    return wa, wb


def kernel(
    sizes, b_hbm, l_hbm, sol_ref, res_ref,
    links, edge_links, field, kv, turned, xbuf, zbuf, zpack, tbuf, tpack, acc, red,
    b_sem, l_sem, sent, got, got_sum, seen_z, seen_x,
):
    nx, nz, nt = sizes
    total_count = nx * nz * nt
    ix, iz, it = lax.axis_index("xy"), lax.axis_index("gz"), lax.axis_index("ta")
    here = (ix * nz + iz) * nt + it
    groups = DOF // 8
    ways = 2 if nx > 2 else 1

    def step(axis_value, by, count):
        return lax.rem(axis_value + (by + count), count)

    def at(x, z, t):
        return (x, z, t)

    line_x = [at(step(ix, d, nx), iz, it) for d in range(1, nx)]
    line_z = [at(ix, step(iz, d, nz), it) for d in range(1, nz)]
    line_t = [at(ix, iz, step(it, d, nt)) for d in range(1, nt)]

    def tell(sem, devices):
        for device in devices:
            pl.semaphore_signal(sem, inc=1, device_id=device, device_id_type=MESH)

    def remote(source, target, send_sem, recv_sem, device):
        return pltpu.make_async_remote_copy(
            src_ref=source, dst_ref=target, send_sem=send_sem, recv_sem=recv_sem,
            device_id=device, device_id_type=MESH,
        )

    barrier = pltpu.get_barrier_semaphore()
    tell(barrier, line_t + line_z + line_x)

    b_copy = pltpu.make_async_copy(b_hbm.at[0, 0, 0], field.at[0], b_sem)
    b_copy.start()
    l_copies = {}
    for number, (k, count) in enumerate(((0, 1), (3, 2), (7, 2), (5, 2), (1, 2))):
        part = pl.ds(k, count)
        l_copies[k] = pltpu.make_async_copy(l_hbm.at[0, 0, 0, part], links.at[part], l_sem.at[number])
        l_copies[k].start(priority=1)

    lane = lax.broadcasted_iota(jnp.int32, (8, 128), 1)
    row8 = lax.broadcasted_iota(jnp.int32, (8, 128), 0)
    in_t = lane % CT
    in_z = (lane // CT) % CZ
    odd = lane % 2 == 1

    def rolled(x, by):
        return pltpu.roll(x, by % S, 1) if by % S else x

    def seat(j):
        return (in_t == 2 * j) | (in_t == (2 * j + CT - 1) % CT)

    seats = [seat(j) for j in range(groups)]

    def tiles(ref, first, count):
        return [ref[pl.ds(first + 8 * j, 8), :] for j in range(count)]

    def halo(n):
        mine = kv.at[n]
        for i in range(2 * RHS):
            rows = tiles(mine, i * DOF, groups)
            packed = None
            for j in range(groups):
                part = jnp.where(odd, rolled(rows[j], 2 * j + CT - 1), rolled(rows[j], 2 * j - CT + 1))
                packed = part if packed is None else jnp.where(seats[j], part, packed)
            tpack[n, pl.ds(8 * i, 8), :] = packed
        for way in (0, 1):
            by = 1 if way else -1
            remote(tpack.at[n], tbuf.at[n, way], sent.at[0], got.at[n, 0], at(ix, iz, step(it, by, nt))).start()
        half = RHS * DOF
        for j in range(half // 8):
            a = mine[pl.ds(8 * j, 8), :]
            b = mine[pl.ds(half + 8 * j, 8), :]
            zpack[n, 0, pl.ds(8 * j, 8), :] = jnp.where(in_z == 0, a, rolled(b, CT))
            zpack[n, 1, pl.ds(8 * j, 8), :] = jnp.where(in_z == 0, rolled(a, -CT), b)
        for way in (0, 1):
            by = 1 if way else -1
            remote(zpack.at[n, way], zbuf.at[n, way], sent.at[1], got.at[n, 1], at(ix, step(iz, by, nz), it)).start()
        for way in range(ways):
            by = 1 if way else -1
            remote(mine, xbuf.at[n, way], sent.at[2], got.at[n, 2], at(step(ix, by, nx), iz, it)).start()

    def receive(n, kind, ref):
        remote(ref, ref, sent.at[kind], got.at[n, kind], (ix, iz, it)).wait_recv()

    def products(passes, fresh, merge=False, final=False):
        def block(c0):
            sums = [[None] * (3 * RHS) for _ in range(4)]
            for link, near in passes:
                for j in range(groups):
                    rows = pl.ds(8 * j, 8)
                    vs = []
                    for r in range(RHS):
                        vr = near[pl.ds(2 * r * DOF + 8 * j, 8), :]
                        vi = near[pl.ds((2 * r + 1) * DOF + 8 * j, 8), :]
                        vs += [vr, vi, vr + vi]
                    for q in range(4):
                        c = c0 + q
                        lr = links[link, 0, c, rows, :]
                        li = links[link, 1, c, rows, :]
                        if merge:
                            lr = lr + links[link + 1, 0, c, rows, :]
                            li = li + links[link + 1, 1, c, rows, :]
                            links[link, 0, c, rows, :] = lr
                            links[link, 1, c, rows, :] = li
                        ls = (lr, li, lr + li)
                        for m in range(3 * RHS):
                            x = ls[m % 3] * vs[m]
                            sums[q][m] = x if sums[q][m] is None else sums[q][m] + x
            out = []
            for q in range(4):
                parts = []
                for r in range(RHS):
                    rr, ii, both = sums[q][3 * r : 3 * r + 3]
                    parts += [rr - ii, both - (rr + ii)]
                if not fresh:
                    parts = [acc[i, c0 + q] + parts[i] for i in range(2 * RHS)]
                out.append(parts)
            return out

        def body(step_number, carry):
            if final:
                c0 = step_number * 8
                out = block(c0) + block(c0 + 4)
                for i in range(2 * RHS):
                    rows = pl.ds(pl.multiple_of(i * DOF + c0, 8), 8)
                    turned[0, rows, :] = fold([out[q][i] for q in range(8)])
            else:
                c0 = step_number * 4
                out = block(c0)
                for q in range(4):
                    for i in range(2 * RHS):
                        acc[i, c0 + q] = out[q][i]
            return carry

        lax.fori_loop(0, DOF // (8 if final else 4), body, 0)

    def split_z():
        def body(c, carry):
            for p in range(2):
                for j in range(groups):
                    rows = pl.ds(8 * j, 8)
                    up, down = links[5, p, c, rows, :], links[6, p, c, rows, :]
                    links[5, p, c, rows, :] = jnp.where(in_z == 0, up, down)
                    links[6, p, c, rows, :] = jnp.where(in_z == 0, down, up)
            return carry

        lax.fori_loop(0, DOF, body, 0, unroll=2)

    def pack_edges():
        last = in_t == CT - 1

        def body(c, carry):
            for p in range(2):
                packed = None
                for j in range(groups):
                    rows = pl.ds(8 * j, 8)
                    part = rolled(jnp.where(last, links[7, p, c, rows, :], links[8, p, c, rows, :]), 2 * j)
                    packed = part if packed is None else jnp.where(seats[j], part, packed)
                edge_links[p, c] = packed
            return carry

        lax.fori_loop(0, DOF, body, 0, unroll=8)

    low4, low2, low1 = row8 < 4, row8 % 4 < 2, row8 % 2 < 1

    def fold(xs):
        ys = [
            jnp.where(low4, xs[i], xs[i + 4]) + pltpu.roll(jnp.where(low4, xs[i + 4], xs[i]), 4, 0)
            for i in range(4)
        ]
        zs = [
            jnp.where(low2, ys[i] + pltpu.roll(ys[i], 6, 0), ys[i + 2] + pltpu.roll(ys[i + 2], 2, 0))
            for i in range(2)
        ]
        return jnp.where(low1, zs[0] + pltpu.roll(zs[0], 7, 0), zs[1] + pltpu.roll(zs[1], 1, 0))

    def shift(n):
        mine = kv.at[n]
        for j in range(E // 8):
            rows = pl.ds(8 * j, 8)
            own = mine[rows, :]
            turned[0, rows, :] = rolled(own, -CZ * CT)
            turned[1, rows, :] = rolled(own, CZ * CT)
            turned[2, rows, :] = jnp.where(in_z == 0, rolled(own, -CT), rolled(own, CT))
            turned[3, rows, :] = jnp.where(in_t == CT - 1, 0.0, rolled(own, -1))
            turned[4, rows, :] = jnp.where(in_t == 0, 0.0, rolled(own, 1))

    local = ((0, None), (3, 0), (4, 1), (7, 3), (8, 4), (5, 2))

    def apply(n):
        shift(n)
        terms = [(link, kv.at[n] if near is None else turned.at[near]) for link, near in local]
        if n == 0:
            l_copies[0].wait()
            l_copies[3].wait()
            products(terms[:3], True)
            l_copies[7].wait()
            products(terms[3:5], False)
            pack_edges()
            l_copies[5].wait()
            split_z()
            products(terms[5:], False)
            pl.semaphore_wait(seen_z, len(line_z))
            tell(seen_x, line_x)
            l_copies[1].wait()
        else:
            products(terms, True)
            early()
        receive(n, 2, xbuf.at[n, pl.ds(0, ways)])
        if nx > 2:
            products(((1, xbuf.at[n, 0]), (2, xbuf.at[n, 1])), False)
        else:
            products(((1, xbuf.at[n, 0]),), False, n == 0)
        receive(n, 1, zbuf.at[n])
        half = RHS * DOF
        for j in range(half // 8):
            p0 = zbuf[n, 0, pl.ds(8 * j, 8), :]
            p1 = zbuf[n, 1, pl.ds(8 * j, 8), :]
            turned[2, pl.ds(8 * j, 8), :] = jnp.where(in_z == 0, p1, rolled(p0, CT))
            turned[2, pl.ds(half + 8 * j, 8), :] = jnp.where(in_z == 0, rolled(p1, -CT), p0)
        products(((6, turned.at[2]),), False, final=True)
        receive(n, 0, tbuf.at[n])
        vs = [
            jnp.where(odd, tbuf[n, 0, pl.ds(8 * i, 8), :], tbuf[n, 1, pl.ds(8 * i, 8), :])
            for i in range(4)
        ]
        for c in range(0, DOF, 8):
            parts = [[] for _ in range(4)]
            for j in range(8):
                lr, li = edge_links[0, c + j], edge_links[1, c + j]
                for r in range(RHS):
                    vr, vi = vs[2 * r], vs[2 * r + 1]
                    parts[2 * r].append(lr * vr - li * vi)
                    parts[2 * r + 1].append(lr * vi + li * vr)
            for i in range(4):
                d = fold(parts[i])
                d = d + rolled(d, -2)
                d = d + rolled(d, -4)
                rows = pl.ds(i * DOF + c, 8)
                kv[n + 1, rows, :] = turned[0, rows, :] + jnp.where(seats[0], d, 0.0)

    def dots(a, b, both):
        out = []
        for r in range(RHS):
            re = im = None
            for j in range(groups):
                ar, ai = (a[pl.ds((2 * r + p) * DOF + 8 * j, 8), :] for p in range(2))
                br, bi = (b[pl.ds((2 * r + p) * DOF + 8 * j, 8), :] for p in range(2))
                x = ar * br + ai * bi
                re = x if re is None else re + x
                if both:
                    x = ar * bi - ai * br
                    im = x if im is None else im + x
            out.append((re, im) if both else (re,))
        return out

    def lane_sums(x):
        return jnp.broadcast_to(jnp.sum(x, axis=1, keepdims=True), (8, 128))

    def early():
        d00, d11, d01 = dots(kv.at[0], kv.at[0], False), dots(kv.at[1], kv.at[1], False), dots(kv.at[0], kv.at[1], True)
        sums = lane_sums(fold([x for r in range(RHS) for x in d00[r] + d11[r] + d01[r]]))
        acc_row = jnp.where(lane == row8, sums, 0.0)
        field[4, pl.ds(0, 8), :] = acc_row

    b_copy.wait()
    kv[0] = field[0].T
    pl.semaphore_wait(barrier, len(line_t) + len(line_z) + len(line_x))
    halo(0)
    tell(seen_z, line_z)
    apply(0)
    halo(1)
    apply(1)

    d02, d12, d22 = dots(kv.at[0], kv.at[2], True), dots(kv.at[1], kv.at[2], True), dots(kv.at[2], kv.at[2], False)
    sums = lane_sums(fold([x for r in range(RHS) for x in d02[r] + d12[r]]))
    a, b = d22[0][0], d22[1][0]
    norms = lane_sums(jnp.where(low4, a + pltpu.roll(a, 4, 0), b + pltpu.roll(b, 4, 0)))
    mine = field[4, pl.ds(0, 8), :] + jnp.where(lane == 8 + row8, sums, 0.0)
    mine = mine + jnp.where(lane == 16 + row8 // 4, norms, 0.0)
    pl.semaphore_wait(seen_x, len(line_x))
    red[here] = jnp.sum(mine, axis=0, keepdims=True)
    for x, z, t in itertools.product(range(nx), range(nz), range(nt)):

        @pl.when((x * nz + z) * nt + t != here)
        def _():
            remote(red.at[here], red.at[here], sent.at[3], got_sum, (x, z, t)).start()

    in_p = (lax.broadcasted_iota(jnp.int32, (S, E), 1) // DOF) % 2

    def aside(v):
        return jnp.where(in_p == 0, pltpu.roll(v, E - DOF, 1), -pltpu.roll(v, DOF, 1))

    k1, k2 = kv[1].T, kv[2].T
    field[1] = k1
    field[2] = k2
    turned[0] = aside(field[0])
    turned[1] = aside(k1)
    turned[2] = aside(k2)
    for kind, ref in ((0, tbuf), (1, zbuf), (2, xbuf.at[:, pl.ds(0, ways)])):
        remote(ref, ref, sent.at[kind], got_sum, (ix, iz, it)).wait_send()

    others = red.at[pl.ds(0, total_count - 1)]
    remote(others, others, sent.at[3], got_sum, (ix, iz, it)).wait_recv()
    value = jnp.broadcast_to(jnp.sum(red[...], axis=0), (8, 128))
    first_half = lane < 2 * DOF

    def pick(place):
        return [jnp.sum(jnp.where(lane == place + by * r, value, 0.0), axis=1, keepdims=True) for r, by in ((0, 0), (1, 4))]

    place = (row8 // 4) * 8 + row8 % 4
    low, high = pick(place)
    gram = jnp.where(first_half, low, high)
    low, _ = pick(16 + row8 * 0)
    high, _ = pick(17 + row8 * 0)
    g22 = jnp.where(first_half, low, high)[0:1]
    g = [gram[i : i + 1] for i in range(8)]
    wa, wb = coefficients(g[0], g[1], g22, (g[2], g[3]), (g[4], g[5]), (g[6], g[7]))

    def weighted(w, v, z):
        return w[0] * v - w[1] * z

    k0, k1, k2 = field[0], field[1], field[2]
    z0, z1, z2 = turned[0], turned[1], turned[2]
    sol = weighted(wa, k0, z0) + weighted(wb, k1, z1)
    image = weighted(wa, k1, z1) + weighted(wb, k2, z2)
    sol_ref[0, 0, 0] = sol
    res_ref[0, 0, 0] = k0 - mass_shift * sol - image
    remote(others, others, sent.at[3], got_sum, (ix, iz, it)).wait_send()


def deliver(a_ref, b_ref, sol_ref, res_ref):
    sol_ref[...] = a_ref[...]
    res_ref[...] = b_ref[...]


def shards(sizes, right_side, link_blocks):
    nx, nz, nt = sizes
    out = jax.ShapeDtypeStruct(right_side.shape, jnp.float32)
    f32 = jnp.float32
    held = pltpu.VMEM(right_side.shape, f32)
    results = pl.pallas_call(
        functools.partial(kernel, sizes),
        out_shape=(held, held),
        in_specs=[pl.BlockSpec(memory_space=pl.ANY)] * 2,
        out_specs=(pl.BlockSpec(memory_space=pltpu.VMEM),) * 2,
        scratch_shapes=[
            pltpu.VMEM((9, 2, DOF, DOF, S), f32),
            pltpu.VMEM((2, DOF, 8, S), f32),
            pltpu.VMEM((5, S, E), f32),
            pltpu.VMEM((3, E, S), f32),
            pltpu.VMEM((5, E, S), f32),
            pltpu.VMEM((2, 2 if nx > 2 else 1, E, S), f32),
            pltpu.VMEM((2, 2, RHS * DOF, S), f32),
            pltpu.VMEM((2, 2, RHS * DOF, S), f32),
            pltpu.VMEM((2, 2, 2 * RHS * 8, S), f32),
            pltpu.VMEM((2, 2 * RHS * 8, S), f32),
            pltpu.VMEM((4, DOF, 8, S), f32),
            pltpu.VMEM((nx * nz * nt, 1, 128), f32),
            pltpu.SemaphoreType.DMA,
            pltpu.SemaphoreType.DMA((5,)),
            pltpu.SemaphoreType.DMA((4,)),
            pltpu.SemaphoreType.DMA((2, 3)),
            pltpu.SemaphoreType.DMA,
            pltpu.SemaphoreType.REGULAR,
            pltpu.SemaphoreType.REGULAR,
        ],
        compiler_params=pltpu.CompilerParams(
            collective_id=0, has_side_effects=True, vmem_limit_bytes=56 * 1024 * 1024
        ),
    )(right_side, link_blocks)
    return pl.pallas_call(
        deliver,
        out_shape=(out, out),
        in_specs=[pl.BlockSpec(memory_space=pltpu.VMEM)] * 2,
        out_specs=(pl.BlockSpec(memory_space=pltpu.VMEM),) * 2,
    )(*[pltpu.with_memory_space_constraint(x, pltpu.VMEM) for x in results])


def solution(mesh):
    sizes = tuple(mesh.shape[name] for name in ("xy", "gz", "ta"))
    return jax.shard_map(
        functools.partial(shards, sizes),
        mesh=mesh,
        in_specs=(
            P("xy", "gz", "ta", None, None),
            P("xy", "gz", "ta", None, None, None, None, None),
        ),
        out_specs=(P("xy", "gz", "ta", None, None), P("xy", "gz", "ta", None, None)),
        check_vma=False,
    )
```

```python
import functools
import itertools

import jax
import jax.numpy as jnp
from jax import lax
from jax.experimental import pallas as pl
from jax.experimental.pallas import tpu as pltpu
from jax.sharding import PartitionSpec as P

DOF = 32
RHS = 2
NY = 8
CZ = 2
CT = 8
S = 128
E = 128
MESH = pl.DeviceIdType.MESH

mass_shift = 4.0
epsilon = 1e-06


def cmul(a, b):
    return (a[0] * b[0] - a[1] * b[1], a[0] * b[1] + a[1] * b[0])


def conj(a):
    return (a[0], -a[1])


def cadd(a, b):
    return (a[0] + b[0], a[1] + b[1])


def csub(a, b):
    return (a[0] - b[0], a[1] - b[1])


def scale(a, x):
    return (a[0] * x, a[1] * x)


def size2(a):
    return a[0] * a[0] + a[1] * a[1]


def coefficients(g00, g11, g22, g01, g02, g12):
    beta2 = g00 + epsilon
    beta = jnp.sqrt(beta2)
    inv_beta2 = 1.0 / beta2
    h00 = scale((mass_shift * g00 + g01[0], g01[1]), inv_beta2)
    a = (mass_shift - h00[0], -h00[1])
    left = g11 + size2(a) * g00 + 2.0 * cmul(conj(a), g01)[0]
    h10_2 = jnp.maximum(left, 0.0) * inv_beta2 + epsilon
    h10 = jnp.sqrt(h10_2)
    a4 = (a[0] + mass_shift, a[1])
    a_4 = scale(a, mass_shift)
    top = cadd(cadd(g02, cmul(a4, g01)), scale(a_4, g00))
    h01 = scale(top, inv_beta2 / h10)
    low = cadd(cadd(g12, scale(a4, g11)), cmul(a_4, conj(g01)))
    h11 = scale(cadd(low, cmul(conj(a), top)), inv_beta2 / h10_2)
    p = csub(a4, h11)
    q = csub(csub(a_4, scale(h01, h10)), cmul(h11, a))
    left = g22 + size2(p) * g11 + size2(q) * g00
    left = left + 2.0 * (
        cmul(p, conj(g12))[0] + cmul(q, conj(g02))[0] + cmul(cmul(conj(q), p), g01)[0]
    )
    h21_2 = jnp.maximum(left, 0.0) * (inv_beta2 / h10_2) + epsilon
    m00 = size2(h00) + h10_2
    m01 = cadd(cmul(conj(h00), h01), scale(h11, h10))
    m11 = size2(h01) + size2(h11) + h21_2
    t0 = scale(conj(h00), beta)
    t1 = scale(conj(h01), beta)
    inv_l0 = 1.0 / jnp.sqrt(m00)
    l10 = scale(conj(m01), inv_l0)
    f0 = scale(t0, inv_l0)
    inv_d = 1.0 / (m11 - size2(l10))
    y1 = scale(csub(t1, cmul(l10, f0)), inv_d)
    y0 = scale(csub(f0, cmul(conj(l10), y1)), inv_l0)
    inv_beta = 1.0 / beta
    wb = scale(y1, inv_beta / h10)
    wa = cadd(scale(y0, inv_beta), cmul(wb, a))
    return wa, wb


def kernel(
    sizes, b_hbm, l_hbm, sol_ref, res_ref,
    links, edge_links, field, kv, turned, xbuf, zbuf, zpack, tbuf, tpack, acc, red,
    b_sem, l_sem, sent, got, got_sum, seen_z, seen_x,
):
    nx, nz, nt = sizes
    total_count = nx * nz * nt
    ix, iz, it = lax.axis_index("xy"), lax.axis_index("gz"), lax.axis_index("ta")
    here = (ix * nz + iz) * nt + it
    groups = DOF // 8
    ways = 2 if nx > 2 else 1

    def step(axis_value, by, count):
        return lax.rem(axis_value + (by + count), count)

    def at(x, z, t):
        return (x, z, t)

    line_x = [at(step(ix, d, nx), iz, it) for d in range(1, nx)]
    line_z = [at(ix, step(iz, d, nz), it) for d in range(1, nz)]
    line_t = [at(ix, iz, step(it, d, nt)) for d in range(1, nt)]

    def tell(sem, devices):
        for device in devices:
            pl.semaphore_signal(sem, inc=1, device_id=device, device_id_type=MESH)

    def remote(source, target, send_sem, recv_sem, device):
        return pltpu.make_async_remote_copy(
            src_ref=source, dst_ref=target, send_sem=send_sem, recv_sem=recv_sem,
            device_id=device, device_id_type=MESH,
        )

    b_copy = pltpu.make_async_copy(b_hbm.at[0, 0, 0], field.at[0], b_sem)
    b_copy.start()

    barrier = pltpu.get_barrier_semaphore()
    tell(barrier, line_t + line_z + line_x)

    l_copies = {}
    for number, (k, count) in enumerate(((0, 1), (3, 2), (7, 2), (5, 2), (1, 2))):
        part = pl.ds(k, count)
        l_copies[k] = pltpu.make_async_copy(l_hbm.at[0, 0, 0, part], links.at[part], l_sem.at[number])
        l_copies[k].start(priority=1)

    lane = lax.broadcasted_iota(jnp.int32, (8, 128), 1)
    row8 = lax.broadcasted_iota(jnp.int32, (8, 128), 0)
    in_t = lane % CT
    in_z = (lane // CT) % CZ
    odd = lane % 2 == 1

    def rolled(x, by):
        return pltpu.roll(x, by % S, 1) if by % S else x

    def seat(j):
        return (in_t == 2 * j) | (in_t == (2 * j + CT - 1) % CT)

    seats = [seat(j) for j in range(groups)]

    def tiles(ref, first, count):
        return [ref[pl.ds(first + 8 * j, 8), :] for j in range(count)]

    def z_rows(h):
        count = groups // 2
        return [(p, h * count + d, (p * count + d) * 8) for p in range(2) for d in range(count)]

    def halo(n):
        mine = kv.at[n]
        for i in range(2 * RHS):
            rows = tiles(mine, i * DOF, groups)
            packed = None
            for j in range(groups):
                part = jnp.where(odd, rolled(rows[j], 2 * j + CT - 1), rolled(rows[j], 2 * j - CT + 1))
                packed = part if packed is None else jnp.where(seats[j], part, packed)
            tpack[n, pl.ds(8 * i, 8), :] = packed
        for way in (0, 1):
            by = 1 if way else -1
            remote(tpack.at[n], tbuf.at[n, way], sent.at[0], got.at[n, 0], at(ix, iz, step(it, by, nt))).start()
        for h in range(2):
            for p, dj, row in z_rows(h):
                a = mine[pl.ds(p * DOF + 8 * dj, 8), :]
                b = mine[pl.ds((2 + p) * DOF + 8 * dj, 8), :]
                zpack[n, h, 0, pl.ds(row, 8), :] = jnp.where(in_z == 0, a, rolled(b, CT))
                zpack[n, h, 1, pl.ds(row, 8), :] = jnp.where(in_z == 0, rolled(a, -CT), b)
            for way in (0, 1):
                by = 1 if way else -1
                remote(
                    zpack.at[n, h, way], zbuf.at[n, h, way], sent.at[1], got.at[n, 2 + h], at(ix, step(iz, by, nz), it)
                ).start()
        for way in range(ways):
            by = 1 if way else -1
            remote(mine, xbuf.at[n, way], sent.at[2], got.at[n, 1], at(step(ix, by, nx), iz, it)).start()

    def receive(n, kind, ref):
        remote(ref, ref, sent.at[0], got.at[n, kind], (ix, iz, it)).wait_recv()

    def products(passes, fresh, merge=False, final=False, span=range(groups)):
        def block(c0):
            sums = [[None] * (3 * RHS) for _ in range(4)]
            for link, near in passes:
                for j in span:
                    rows = pl.ds(8 * j, 8)
                    vs = []
                    for r in range(RHS):
                        vr = near[pl.ds(2 * r * DOF + 8 * j, 8), :]
                        vi = near[pl.ds((2 * r + 1) * DOF + 8 * j, 8), :]
                        vs += [vr, vi, vr + vi]
                    for q in range(4):
                        c = c0 + q
                        lr = links[link, 0, c, rows, :]
                        li = links[link, 1, c, rows, :]
                        if merge:
                            lr = lr + links[link + 1, 0, c, rows, :]
                            li = li + links[link + 1, 1, c, rows, :]
                            links[link, 0, c, rows, :] = lr
                            links[link, 1, c, rows, :] = li
                        ls = (lr, li, lr + li)
                        for m in range(3 * RHS):
                            x = ls[m % 3] * vs[m]
                            sums[q][m] = x if sums[q][m] is None else sums[q][m] + x
            out = []
            for q in range(4):
                parts = []
                for r in range(RHS):
                    rr, ii, both = sums[q][3 * r : 3 * r + 3]
                    parts += [rr - ii, both - (rr + ii)]
                if not fresh:
                    parts = [acc[i, c0 + q] + parts[i] for i in range(2 * RHS)]
                out.append(parts)
            return out

        def body(step_number, carry):
            if final:
                c0 = step_number * 8
                out = block(c0) + block(c0 + 4)
                for i in range(2 * RHS):
                    rows = pl.ds(pl.multiple_of(i * DOF + c0, 8), 8)
                    turned[0, rows, :] = turned[0, rows, :] + fold([out[q][i] for q in range(8)])
            else:
                c0 = step_number * 4
                out = block(c0)
                for q in range(4):
                    for i in range(2 * RHS):
                        acc[i, c0 + q] = out[q][i]
            return carry

        lax.fori_loop(0, DOF // (8 if final else 4), body, 0)

    def split_z():
        def body(c, carry):
            for p in range(2):
                for j in range(groups):
                    rows = pl.ds(8 * j, 8)
                    up, down = links[5, p, c, rows, :], links[6, p, c, rows, :]
                    links[5, p, c, rows, :] = jnp.where(in_z == 0, up, down)
                    links[6, p, c, rows, :] = jnp.where(in_z == 0, down, up)
            return carry

        lax.fori_loop(0, DOF, body, 0, unroll=2)

    def pack_edges():
        last = in_t == CT - 1

        def body(c, carry):
            for p in range(2):
                packed = None
                for j in range(groups):
                    rows = pl.ds(8 * j, 8)
                    part = rolled(jnp.where(last, links[7, p, c, rows, :], links[8, p, c, rows, :]), 2 * j)
                    packed = part if packed is None else jnp.where(seats[j], part, packed)
                edge_links[p, c] = packed
            return carry

        lax.fori_loop(0, DOF, body, 0, unroll=8)

    low4, low2, low1 = row8 < 4, row8 % 4 < 2, row8 % 2 < 1

    def fold(xs):
        ys = [
            jnp.where(low4, xs[i], xs[i + 4]) + pltpu.roll(jnp.where(low4, xs[i + 4], xs[i]), 4, 0)
            for i in range(4)
        ]
        zs = [
            jnp.where(low2, ys[i] + pltpu.roll(ys[i], 6, 0), ys[i + 2] + pltpu.roll(ys[i + 2], 2, 0))
            for i in range(2)
        ]
        return jnp.where(low1, zs[0] + pltpu.roll(zs[0], 7, 0), zs[1] + pltpu.roll(zs[1], 1, 0))

    def shift(n):
        mine = kv.at[n]
        for j in range(E // 8):
            rows = pl.ds(8 * j, 8)
            own = mine[rows, :]
            turned[0, rows, :] = rolled(own, -CZ * CT)
            turned[1, rows, :] = rolled(own, CZ * CT)
            turned[2, rows, :] = jnp.where(in_z == 0, rolled(own, -CT), rolled(own, CT))
            turned[3, rows, :] = jnp.where(in_t == CT - 1, 0.0, rolled(own, -1))
            turned[4, rows, :] = jnp.where(in_t == 0, 0.0, rolled(own, 1))

    local = ((0, None), (3, 0), (4, 1), (7, 3), (8, 4), (5, 2))

    def apply(n):
        shift(n)
        terms = [(link, kv.at[n] if near is None else turned.at[near]) for link, near in local]
        if n == 0:
            l_copies[0].wait()
            l_copies[3].wait()
            products(terms[:3], True)
            l_copies[7].wait()
            products(terms[3:5], False)
            pack_edges()
            l_copies[5].wait()
            split_z()
            products(terms[5:], False)
            pl.semaphore_wait(seen_z, len(line_z))
            tell(seen_x, line_x)
            l_copies[1].wait()
        else:
            products(terms, True)
            early()
        receive(n, 1, xbuf.at[n, pl.ds(0, ways)])
        if nx > 2:
            products(((1, xbuf.at[n, 0]), (2, xbuf.at[n, 1])), False)
        else:
            products(((1, xbuf.at[n, 0]),), False, n == 0)
        for h in range(2):
            receive(n, 2 + h, zbuf.at[n, h])
            for p, dj, row in z_rows(h):
                p0 = zbuf[n, h, 0, pl.ds(row, 8), :]
                p1 = zbuf[n, h, 1, pl.ds(row, 8), :]
                turned[2, pl.ds(p * DOF + 8 * dj, 8), :] = jnp.where(in_z == 0, p1, rolled(p0, CT))
                turned[2, pl.ds((2 + p) * DOF + 8 * dj, 8), :] = jnp.where(in_z == 0, rolled(p1, -CT), p0)
            span = range(h * groups // 2, (h + 1) * groups // 2)
            products(((6, turned.at[2]),), h == 1, final=h == 1, span=span)
            if h == 0:
                for i in range(4):
                    for c in range(0, DOF, 8):
                        turned[0, pl.ds(i * DOF + c, 8), :] = fold([acc[i, c + j] for j in range(8)])
        receive(n, 0, tbuf.at[n])
        vs = [
            jnp.where(odd, tbuf[n, 0, pl.ds(8 * i, 8), :], tbuf[n, 1, pl.ds(8 * i, 8), :])
            for i in range(4)
        ]
        for c in range(0, DOF, 8):
            parts = [[] for _ in range(4)]
            for j in range(8):
                lr, li = edge_links[0, c + j], edge_links[1, c + j]
                for r in range(RHS):
                    vr, vi = vs[2 * r], vs[2 * r + 1]
                    parts[2 * r].append(lr * vr - li * vi)
                    parts[2 * r + 1].append(lr * vi + li * vr)
            for i in range(4):
                d = fold(parts[i])
                d = (d + rolled(d, -2)) + (rolled(d, -4) + rolled(d, -6))
                rows = pl.ds(i * DOF + c, 8)
                kv[n + 1, rows, :] = turned[0, rows, :] + jnp.where(seats[0], d, 0.0)

    def dots(a, b, both):
        out = []
        for r in range(RHS):
            re = im = None
            for j in range(groups):
                ar, ai = (a[pl.ds((2 * r + p) * DOF + 8 * j, 8), :] for p in range(2))
                br, bi = (b[pl.ds((2 * r + p) * DOF + 8 * j, 8), :] for p in range(2))
                x = ar * br + ai * bi
                re = x if re is None else re + x
                if both:
                    x = ar * bi - ai * br
                    im = x if im is None else im + x
            out.append((re, im) if both else (re,))
        return out

    def lane_sums(x):
        return jnp.broadcast_to(jnp.sum(x, axis=1, keepdims=True), (8, 128))

    def early():
        d00, d11, d01 = dots(kv.at[0], kv.at[0], False), dots(kv.at[1], kv.at[1], False), dots(kv.at[0], kv.at[1], True)
        sums = lane_sums(fold([x for r in range(RHS) for x in d00[r] + d11[r] + d01[r]]))
        acc_row = jnp.where(lane == row8, sums, 0.0)
        field[4, pl.ds(0, 8), :] = acc_row

    b_copy.wait()
    kv[0] = field[0].T
    pl.semaphore_wait(barrier, len(line_t) + len(line_z) + len(line_x))
    halo(0)
    tell(seen_z, line_z)
    apply(0)
    halo(1)
    apply(1)

    d02, d12, d22 = dots(kv.at[0], kv.at[2], True), dots(kv.at[1], kv.at[2], True), dots(kv.at[2], kv.at[2], False)
    sums = lane_sums(fold([x for r in range(RHS) for x in d02[r] + d12[r]]))
    a, b = d22[0][0], d22[1][0]
    norms = lane_sums(jnp.where(low4, a + pltpu.roll(a, 4, 0), b + pltpu.roll(b, 4, 0)))
    mine = field[4, pl.ds(0, 8), :] + jnp.where(lane == 8 + row8, sums, 0.0)
    mine = mine + jnp.where(lane == 16 + row8 // 4, norms, 0.0)
    pl.semaphore_wait(seen_x, len(line_x))
    red[here] = jnp.sum(mine, axis=0, keepdims=True)
    for x, z, t in itertools.product(range(nx), range(nz), range(nt)):

        @pl.when((x * nz + z) * nt + t != here)
        def _():
            remote(red.at[here], red.at[here], sent.at[3], got_sum, (x, z, t)).start()

    in_p = (lax.broadcasted_iota(jnp.int32, (S, E), 1) // DOF) % 2

    def aside(v):
        return jnp.where(in_p == 0, pltpu.roll(v, E - DOF, 1), -pltpu.roll(v, DOF, 1))

    k1, k2 = kv[1].T, kv[2].T
    field[1] = k1
    field[2] = k2
    turned[0] = aside(field[0])
    turned[1] = aside(k1)
    turned[2] = aside(k2)
    for kind, ref in ((0, tbuf), (1, zbuf), (2, xbuf.at[:, pl.ds(0, ways)])):
        remote(ref, ref, sent.at[kind], got_sum, (ix, iz, it)).wait_send()

    others = red.at[pl.ds(0, total_count - 1)]
    remote(others, others, sent.at[3], got_sum, (ix, iz, it)).wait_recv()
    value = jnp.broadcast_to(jnp.sum(red[...], axis=0), (8, 128))
    first_half = lane < 2 * DOF

    def pick(place):
        return [jnp.sum(jnp.where(lane == place + by * r, value, 0.0), axis=1, keepdims=True) for r, by in ((0, 0), (1, 4))]

    place = (row8 // 4) * 8 + row8 % 4
    low, high = pick(place)
    gram = jnp.where(first_half, low, high)
    low, _ = pick(16 + row8 * 0)
    high, _ = pick(17 + row8 * 0)
    g22 = jnp.where(first_half, low, high)[0:1]
    g = [gram[i : i + 1] for i in range(8)]
    wa, wb = coefficients(g[0], g[1], g22, (g[2], g[3]), (g[4], g[5]), (g[6], g[7]))

    def weighted(w, v, z):
        return w[0] * v - w[1] * z

    k0, k1, k2 = field[0], field[1], field[2]
    z0, z1, z2 = turned[0], turned[1], turned[2]
    sol = weighted(wa, k0, z0) + weighted(wb, k1, z1)
    image = weighted(wa, k1, z1) + weighted(wb, k2, z2)
    sol_ref[0, 0, 0] = sol
    res_ref[0, 0, 0] = k0 - mass_shift * sol - image
    remote(others, others, sent.at[3], got_sum, (ix, iz, it)).wait_send()


def deliver(a_ref, b_ref, sol_ref, res_ref):
    sol_ref[...] = a_ref[...]
    res_ref[...] = b_ref[...]


def shards(sizes, right_side, link_blocks):
    nx, nz, nt = sizes
    out = jax.ShapeDtypeStruct(right_side.shape, jnp.float32)
    f32 = jnp.float32
    held = pltpu.VMEM(right_side.shape, f32)
    results = pl.pallas_call(
        functools.partial(kernel, sizes),
        out_shape=(held, held),
        in_specs=[pl.BlockSpec(memory_space=pl.ANY)] * 2,
        out_specs=(pl.BlockSpec(memory_space=pltpu.VMEM),) * 2,
        scratch_shapes=[
            pltpu.VMEM((9, 2, DOF, DOF, S), f32),
            pltpu.VMEM((2, DOF, 8, S), f32),
            pltpu.VMEM((5, S, E), f32),
            pltpu.VMEM((3, E, S), f32),
            pltpu.VMEM((5, E, S), f32),
            pltpu.VMEM((2, 2 if nx > 2 else 1, E, S), f32),
            pltpu.VMEM((2, 2, 2, DOF, S), f32),
            pltpu.VMEM((2, 2, 2, DOF, S), f32),
            pltpu.VMEM((2, 2, 2 * RHS * 8, S), f32),
            pltpu.VMEM((2, 2 * RHS * 8, S), f32),
            pltpu.VMEM((4, DOF, 8, S), f32),
            pltpu.VMEM((nx * nz * nt, 1, 128), f32),
            pltpu.SemaphoreType.DMA,
            pltpu.SemaphoreType.DMA((5,)),
            pltpu.SemaphoreType.DMA((4,)),
            pltpu.SemaphoreType.DMA((2, 4)),
            pltpu.SemaphoreType.DMA,
            pltpu.SemaphoreType.REGULAR,
            pltpu.SemaphoreType.REGULAR,
        ],
        compiler_params=pltpu.CompilerParams(
            collective_id=0, has_side_effects=True, vmem_limit_bytes=56 * 1024 * 1024
        ),
    )(right_side, link_blocks)
    return pl.pallas_call(
        deliver,
        out_shape=(out, out),
        in_specs=[pl.BlockSpec(memory_space=pltpu.VMEM)] * 2,
        out_specs=(pl.BlockSpec(memory_space=pltpu.VMEM),) * 2,
    )(*[pltpu.with_memory_space_constraint(x, pltpu.VMEM) for x in results])


def solution(mesh):
    sizes = tuple(mesh.shape[name] for name in ("xy", "gz", "ta"))
    return jax.shard_map(
        functools.partial(shards, sizes),
        mesh=mesh,
        in_specs=(
            P("xy", "gz", "ta", None, None),
            P("xy", "gz", "ta", None, None, None, None, None),
        ),
        out_specs=(P("xy", "gz", "ta", None, None), P("xy", "gz", "ta", None, None)),
        check_vma=False,
    )
```

```python
import functools
import itertools

import jax
import jax.numpy as jnp
from jax import lax
from jax.experimental import pallas as pl
from jax.experimental.pallas import tpu as pltpu
from jax.sharding import PartitionSpec as P

DOF = 32
RHS = 2
NY = 8
CZ = 2
CT = 8
S = 128
E = 128
MESH = pl.DeviceIdType.MESH

mass_shift = 4.0
epsilon = 1e-06


def cmul(a, b):
    return (a[0] * b[0] - a[1] * b[1], a[0] * b[1] + a[1] * b[0])


def conj(a):
    return (a[0], -a[1])


def cadd(a, b):
    return (a[0] + b[0], a[1] + b[1])


def csub(a, b):
    return (a[0] - b[0], a[1] - b[1])


def scale(a, x):
    return (a[0] * x, a[1] * x)


def size2(a):
    return a[0] * a[0] + a[1] * a[1]


def coefficients(g00, g11, g22, g01, g02, g12):
    beta2 = g00 + epsilon
    beta = jnp.sqrt(beta2)
    inv_beta2 = 1.0 / beta2
    h00 = scale((mass_shift * g00 + g01[0], g01[1]), inv_beta2)
    a = (mass_shift - h00[0], -h00[1])
    left = g11 + size2(a) * g00 + 2.0 * cmul(conj(a), g01)[0]
    h10_2 = jnp.maximum(left, 0.0) * inv_beta2 + epsilon
    h10 = jnp.sqrt(h10_2)
    a4 = (a[0] + mass_shift, a[1])
    a_4 = scale(a, mass_shift)
    top = cadd(cadd(g02, cmul(a4, g01)), scale(a_4, g00))
    h01 = scale(top, inv_beta2 / h10)
    low = cadd(cadd(g12, scale(a4, g11)), cmul(a_4, conj(g01)))
    h11 = scale(cadd(low, cmul(conj(a), top)), inv_beta2 / h10_2)
    p = csub(a4, h11)
    q = csub(csub(a_4, scale(h01, h10)), cmul(h11, a))
    left = g22 + size2(p) * g11 + size2(q) * g00
    left = left + 2.0 * (
        cmul(p, conj(g12))[0] + cmul(q, conj(g02))[0] + cmul(cmul(conj(q), p), g01)[0]
    )
    h21_2 = jnp.maximum(left, 0.0) * (inv_beta2 / h10_2) + epsilon
    m00 = size2(h00) + h10_2
    m01 = cadd(cmul(conj(h00), h01), scale(h11, h10))
    m11 = size2(h01) + size2(h11) + h21_2
    t0 = scale(conj(h00), beta)
    t1 = scale(conj(h01), beta)
    inv_l0 = 1.0 / jnp.sqrt(m00)
    l10 = scale(conj(m01), inv_l0)
    f0 = scale(t0, inv_l0)
    inv_d = 1.0 / (m11 - size2(l10))
    y1 = scale(csub(t1, cmul(l10, f0)), inv_d)
    y0 = scale(csub(f0, cmul(conj(l10), y1)), inv_l0)
    inv_beta = 1.0 / beta
    wb = scale(y1, inv_beta / h10)
    wa = cadd(scale(y0, inv_beta), cmul(wb, a))
    return wa, wb


def kernel(
    sizes, b_hbm, l_hbm, sol_ref, res_ref,
    links, edge_links, z_links, rows, field, kv, turned, xbuf, zbuf, zpack, tbuf, tpack, acc, red,
    b_sem, l_sem, sent, got, got_sum, seen_z, seen_x,
):
    nx, nz, nt = sizes
    total_count = nx * nz * nt
    ix, iz, it = lax.axis_index("xy"), lax.axis_index("gz"), lax.axis_index("ta")
    here = (ix * nz + iz) * nt + it
    groups = DOF // 8
    ways = 2 if nx > 2 else 1

    def step(axis_value, by, count):
        return lax.rem(axis_value + (by + count), count)

    def at(x, z, t):
        return (x, z, t)

    line_x = [at(step(ix, d, nx), iz, it) for d in range(1, nx)]
    line_z = [at(ix, step(iz, d, nz), it) for d in range(1, nz)]
    line_t = [at(ix, iz, step(it, d, nt)) for d in range(1, nt)]

    def tell(sem, devices):
        for device in devices:
            pl.semaphore_signal(sem, inc=1, device_id=device, device_id_type=MESH)

    def remote(source, target, send_sem, recv_sem, device):
        return pltpu.make_async_remote_copy(
            src_ref=source, dst_ref=target, send_sem=send_sem, recv_sem=recv_sem,
            device_id=device, device_id_type=MESH,
        )

    b_copy = pltpu.make_async_copy(b_hbm.at[0, 0, 0], field.at[0], b_sem)
    b_copy.start()

    barrier = pltpu.get_barrier_semaphore()
    tell(barrier, line_t + line_z + line_x)

    l_copies = {}
    for number, (k, count) in enumerate(((0, 1), (3, 2), (7, 2), (5, 2), (1, 2))):
        part = pl.ds(k, count)
        l_copies[k] = pltpu.make_async_copy(l_hbm.at[0, 0, 0, part], links.at[part], l_sem.at[number])
        l_copies[k].start(priority=1)

    lane = lax.broadcasted_iota(jnp.int32, (8, 128), 1)
    row8 = lax.broadcasted_iota(jnp.int32, (8, 128), 0)
    in_t = lane % CT
    in_z = (lane // CT) % CZ
    odd = lane % 2 == 1

    def rolled(x, by):
        return pltpu.roll(x, by % S, 1) if by % S else x

    def seat(j):
        return (in_t == 2 * j) | (in_t == (2 * j + CT - 1) % CT)

    seats = [seat(j) for j in range(groups)]

    def tiles(ref, first, count):
        return [ref[pl.ds(first + 8 * j, 8), :] for j in range(count)]

    def z_rows(h):
        count = groups // 2
        return [(p, h * count + d, (p * count + d) * 8) for p in range(2) for d in range(count)]

    def halo(n):
        mine = kv.at[n]
        for i in range(2 * RHS):
            rows = tiles(mine, i * DOF, groups)
            packed = None
            for j in range(groups):
                part = jnp.where(odd, rolled(rows[j], 2 * j + CT - 1), rolled(rows[j], 2 * j - CT + 1))
                packed = part if packed is None else jnp.where(seats[j], part, packed)
            tpack[n, pl.ds(8 * i, 8), :] = packed
        for way in (0, 1):
            by = 1 if way else -1
            remote(tpack.at[n], tbuf.at[n, way], sent.at[0], got.at[n, 0], at(ix, iz, step(it, by, nt))).start()
        for h in range(2):
            for p, dj, row in z_rows(h):
                a = mine[pl.ds(p * DOF + 8 * dj, 8), :]
                b = mine[pl.ds((2 + p) * DOF + 8 * dj, 8), :]
                zpack[n, h, 0, pl.ds(row, 8), :] = jnp.where(in_z == 0, a, rolled(b, CT))
                zpack[n, h, 1, pl.ds(row, 8), :] = jnp.where(in_z == 0, rolled(a, -CT), b)
            for way in (0, 1):
                by = 1 if way else -1
                remote(
                    zpack.at[n, h, way], zbuf.at[n, h, way], sent.at[1], got.at[n, 2 + h], at(ix, step(iz, by, nz), it)
                ).start()
        for way in range(ways):
            by = 1 if way else -1
            remote(mine, xbuf.at[n, way], sent.at[2], got.at[n, 1], at(step(ix, by, nx), iz, it)).start()

    def receive(n, kind, ref):
        remote(ref, ref, sent.at[0], got.at[n, kind], (ix, iz, it)).wait_recv()

    def products(passes, fresh, merge=False):
        def block(c0):
            sums = [[None] * (3 * RHS) for _ in range(4)]
            for link, near in passes:
                for j in range(groups):
                    rows = pl.ds(8 * j, 8)
                    vs = []
                    for r in range(RHS):
                        vr = near[pl.ds(2 * r * DOF + 8 * j, 8), :]
                        vi = near[pl.ds((2 * r + 1) * DOF + 8 * j, 8), :]
                        vs += [vr, vi, vr + vi]
                    for q in range(4):
                        c = c0 + q
                        lr = links[link, 0, c, rows, :]
                        li = links[link, 1, c, rows, :]
                        if merge:
                            lr = lr + links[link + 1, 0, c, rows, :]
                            li = li + links[link + 1, 1, c, rows, :]
                            links[link, 0, c, rows, :] = lr
                            links[link, 1, c, rows, :] = li
                        ls = (lr, li, lr + li)
                        for m in range(3 * RHS):
                            x = ls[m % 3] * vs[m]
                            sums[q][m] = x if sums[q][m] is None else sums[q][m] + x
            out = []
            for q in range(4):
                parts = []
                for r in range(RHS):
                    rr, ii, both = sums[q][3 * r : 3 * r + 3]
                    parts += [rr - ii, both - (rr + ii)]
                if not fresh:
                    parts = [acc[i, c0 + q] + parts[i] for i in range(2 * RHS)]
                out.append(parts)
            return out

        def body(step_number, carry):
            c0 = step_number * 4
            out = block(c0)
            for q in range(4):
                for i in range(2 * RHS):
                    acc[i, c0 + q] = out[q][i]
            return carry

        lax.fori_loop(0, DOF // 4, body, 0)

    def split_z():
        def body(c, carry):
            for p in range(2):
                for j in range(groups):
                    rows = pl.ds(8 * j, 8)
                    up, down = links[5, p, c, rows, :], links[6, p, c, rows, :]
                    links[5, p, c, rows, :] = jnp.where(in_z == 0, up, down)
                    z_links[p, pl.ds(c * (DOF + 1) + 8 * j, 8), :] = jnp.where(in_z == 0, down, up)
            return carry

        lax.fori_loop(0, DOF, body, 0, unroll=2)

    def pack_edges():
        last = in_t == CT - 1

        def body(c, carry):
            for p in range(2):
                packed = None
                for j in range(groups):
                    rows = pl.ds(8 * j, 8)
                    part = rolled(jnp.where(last, links[7, p, c, rows, :], links[8, p, c, rows, :]), 2 * j)
                    packed = part if packed is None else jnp.where(seats[j], part, packed)
                edge_links[p, pl.ds(pl.multiple_of(8 * c, 8), 8), :] = packed
            return carry

        lax.fori_loop(0, DOF, body, 0, unroll=8)

    low4, low2, low1 = row8 < 4, row8 % 4 < 2, row8 % 2 < 1

    def fold(xs):
        ys = [
            jnp.where(low4, xs[i], xs[i + 4]) + pltpu.roll(jnp.where(low4, xs[i + 4], xs[i]), 4, 0)
            for i in range(4)
        ]
        zs = [
            jnp.where(low2, ys[i] + pltpu.roll(ys[i], 6, 0), ys[i + 2] + pltpu.roll(ys[i + 2], 2, 0))
            for i in range(2)
        ]
        return jnp.where(low1, zs[0] + pltpu.roll(zs[0], 7, 0), zs[1] + pltpu.roll(zs[1], 1, 0))

    def shift(n):
        mine = kv.at[n]
        for j in range(E // 8):
            rows = pl.ds(8 * j, 8)
            own = mine[rows, :]
            turned[0, rows, :] = rolled(own, -CZ * CT)
            turned[1, rows, :] = rolled(own, CZ * CT)
            turned[2, rows, :] = jnp.where(in_z == 0, rolled(own, -CT), rolled(own, CT))
            turned[3, rows, :] = jnp.where(in_t == CT - 1, 0.0, rolled(own, -1))
            turned[4, rows, :] = jnp.where(in_t == 0, 0.0, rolled(own, 1))

    def row_products(link_at, row_at, steps):
        sums = [[None] * groups for _ in range(3 * RHS)]
        for d in steps:
            vs = [jnp.broadcast_to(row_at(m, d), (8, 128)) for m in range(3 * RHS)]
            for g in range(groups):
                lr, li = link_at(0, g, d), link_at(1, g, d)
                ls = (lr, li, lr + li)
                for m in range(3 * RHS):
                    x = ls[m % 3] * vs[m]
                    sums[m][g] = x if sums[m][g] is None else sums[m][g] + x
        out = []
        for r in range(RHS):
            rr, ii, both = sums[3 * r : 3 * r + 3]
            out.append([rr[g] - ii[g] for g in range(groups)])
            out.append([both[g] - (rr[g] + ii[g]) for g in range(groups)])
        return out

    local = ((0, None), (3, 0), (4, 1), (7, 3), (8, 4), (5, 2))

    def apply(n):
        shift(n)
        terms = [(link, kv.at[n] if near is None else turned.at[near]) for link, near in local]
        if n == 0:
            l_copies[0].wait()
            l_copies[3].wait()
            products(terms[:3], True)
            l_copies[7].wait()
            products(terms[3:5], False)
            pack_edges()
            l_copies[5].wait()
            split_z()
            products(terms[5:], False)
            pl.semaphore_wait(seen_z, len(line_z))
            tell(seen_x, line_x)
            l_copies[1].wait()
        else:
            products(terms, True)
            early()
        receive(n, 1, xbuf.at[n, pl.ds(0, ways)])
        if nx > 2:
            products(((1, xbuf.at[n, 0]), (2, xbuf.at[n, 1])), False)
        else:
            products(((1, xbuf.at[n, 0]),), False, n == 0)
        for i in range(4):
            for c in range(0, DOF, 8):
                turned[0, pl.ds(i * DOF + c, 8), :] = fold([acc[i, c + j] for j in range(8)])
        for h in range(2):
            receive(n, 2 + h, zbuf.at[n, h])
            near = {}
            for p, dj, row in z_rows(h):
                p0 = zbuf[n, h, 0, pl.ds(row, 8), :]
                p1 = zbuf[n, h, 1, pl.ds(row, 8), :]
                near[0, p, dj] = jnp.where(in_z == 0, p1, rolled(p0, CT))
                near[1, p, dj] = jnp.where(in_z == 0, rolled(p1, -CT), p0)
            for r, p, dj in near:
                rows[3 * r + p, pl.ds(8 * dj, 8), :] = near[r, p, dj]
                if p == 0:
                    rows[3 * r + 2, pl.ds(8 * dj, 8), :] = near[r, 0, dj] + near[r, 1, dj]
            got_z = row_products(
                lambda p, g, d: z_links[p, pl.ds(8 * g * (DOF + 1) + d, 8, stride=DOF + 1), :],
                lambda m, d: rows[m, pl.ds(d, 1), :],
                range(h * DOF // 2, (h + 1) * DOF // 2),
            )
            for i in range(4):
                for g in range(groups):
                    place = pl.ds(i * DOF + 8 * g, 8)
                    turned[0, place, :] = turned[0, place, :] + got_z[i][g]
        receive(n, 0, tbuf.at[n])
        for r in range(RHS):
            vr, vi = (
                jnp.where(odd, tbuf[n, 0, pl.ds(8 * i, 8), :], tbuf[n, 1, pl.ds(8 * i, 8), :])
                for i in (2 * r, 2 * r + 1)
            )
            for m, v in enumerate((vr, vi, vr + vi)):
                rows[3 * r + m, pl.ds(DOF, 8), :] = v
        got_t = row_products(
            lambda p, g, d: edge_links[p, pl.ds(64 * g + d, 8, stride=8), :],
            lambda m, d: rows[m, pl.ds(DOF + d, 1), :],
            range(8),
        )
        for i in range(4):
            for g in range(groups):
                d = got_t[i][g]
                d = (d + rolled(d, -2)) + (rolled(d, -4) + rolled(d, -6))
                place = pl.ds(i * DOF + 8 * g, 8)
                kv[n + 1, place, :] = turned[0, place, :] + jnp.where(seats[0], d, 0.0)

    def dots(a, b, both):
        out = []
        for r in range(RHS):
            re = im = None
            for j in range(groups):
                ar, ai = (a[pl.ds((2 * r + p) * DOF + 8 * j, 8), :] for p in range(2))
                br, bi = (b[pl.ds((2 * r + p) * DOF + 8 * j, 8), :] for p in range(2))
                x = ar * br + ai * bi
                re = x if re is None else re + x
                if both:
                    x = ar * bi - ai * br
                    im = x if im is None else im + x
            out.append((re, im) if both else (re,))
        return out

    def lane_sums(x):
        return jnp.broadcast_to(jnp.sum(x, axis=1, keepdims=True), (8, 128))

    def early():
        d00, d11, d01 = dots(kv.at[0], kv.at[0], False), dots(kv.at[1], kv.at[1], False), dots(kv.at[0], kv.at[1], True)
        sums = lane_sums(fold([x for r in range(RHS) for x in d00[r] + d11[r] + d01[r]]))
        acc_row = jnp.where(lane == row8, sums, 0.0)
        field[4, pl.ds(0, 8), :] = acc_row

    b_copy.wait()
    kv[0] = field[0].T
    pl.semaphore_wait(barrier, len(line_t) + len(line_z) + len(line_x))
    halo(0)
    tell(seen_z, line_z)
    apply(0)
    halo(1)
    apply(1)

    d02, d12, d22 = dots(kv.at[0], kv.at[2], True), dots(kv.at[1], kv.at[2], True), dots(kv.at[2], kv.at[2], False)
    sums = lane_sums(fold([x for r in range(RHS) for x in d02[r] + d12[r]]))
    a, b = d22[0][0], d22[1][0]
    norms = lane_sums(jnp.where(low4, a + pltpu.roll(a, 4, 0), b + pltpu.roll(b, 4, 0)))
    mine = field[4, pl.ds(0, 8), :] + jnp.where(lane == 8 + row8, sums, 0.0)
    mine = mine + jnp.where(lane == 16 + row8 // 4, norms, 0.0)
    pl.semaphore_wait(seen_x, len(line_x))
    red[here] = jnp.sum(mine, axis=0, keepdims=True)
    for x, z, t in itertools.product(range(nx), range(nz), range(nt)):

        @pl.when((x * nz + z) * nt + t != here)
        def _():
            remote(red.at[here], red.at[here], sent.at[3], got_sum, (x, z, t)).start()

    in_p = (lax.broadcasted_iota(jnp.int32, (S, E), 1) // DOF) % 2

    def aside(v):
        return jnp.where(in_p == 0, pltpu.roll(v, E - DOF, 1), -pltpu.roll(v, DOF, 1))

    k1, k2 = kv[1].T, kv[2].T
    field[1] = k1
    field[2] = k2
    turned[0] = aside(field[0])
    turned[1] = aside(k1)
    turned[2] = aside(k2)
    for kind, ref in ((0, tbuf), (1, zbuf), (2, xbuf.at[:, pl.ds(0, ways)])):
        remote(ref, ref, sent.at[kind], got_sum, (ix, iz, it)).wait_send()

    others = red.at[pl.ds(0, total_count - 1)]
    remote(others, others, sent.at[3], got_sum, (ix, iz, it)).wait_recv()
    value = jnp.broadcast_to(jnp.sum(red[...], axis=0), (8, 128))
    first_half = lane < 2 * DOF

    def pick(place):
        return [jnp.sum(jnp.where(lane == place + by * r, value, 0.0), axis=1, keepdims=True) for r, by in ((0, 0), (1, 4))]

    place = (row8 // 4) * 8 + row8 % 4
    low, high = pick(place)
    gram = jnp.where(first_half, low, high)
    low, _ = pick(16 + row8 * 0)
    high, _ = pick(17 + row8 * 0)
    g22 = jnp.where(first_half, low, high)[0:1]
    g = [gram[i : i + 1] for i in range(8)]
    wa, wb = coefficients(g[0], g[1], g22, (g[2], g[3]), (g[4], g[5]), (g[6], g[7]))

    def weighted(w, v, z):
        return w[0] * v - w[1] * z

    k0, k1, k2 = field[0], field[1], field[2]
    z0, z1, z2 = turned[0], turned[1], turned[2]
    sol = weighted(wa, k0, z0) + weighted(wb, k1, z1)
    image = weighted(wa, k1, z1) + weighted(wb, k2, z2)
    sol_ref[0, 0, 0] = sol
    res_ref[0, 0, 0] = k0 - mass_shift * sol - image
    remote(others, others, sent.at[3], got_sum, (ix, iz, it)).wait_send()


def deliver(a_ref, b_ref, sol_ref, res_ref):
    sol_ref[...] = a_ref[...]
    res_ref[...] = b_ref[...]


def shards(sizes, right_side, link_blocks):
    nx, nz, nt = sizes
    out = jax.ShapeDtypeStruct(right_side.shape, jnp.float32)
    f32 = jnp.float32
    held = pltpu.VMEM(right_side.shape, f32)
    results = pl.pallas_call(
        functools.partial(kernel, sizes),
        out_shape=(held, held),
        in_specs=[pl.BlockSpec(memory_space=pl.ANY)] * 2,
        out_specs=(pl.BlockSpec(memory_space=pltpu.VMEM),) * 2,
        scratch_shapes=[
            pltpu.VMEM((9, 2, DOF, DOF, S), f32),
            pltpu.VMEM((2, DOF * 8, S), f32),
            pltpu.VMEM((2, DOF * (DOF + 1), S), f32),
            pltpu.VMEM((3 * RHS, DOF + 8, S), f32),
            pltpu.VMEM((5, S, E), f32),
            pltpu.VMEM((3, E, S), f32),
            pltpu.VMEM((5, E, S), f32),
            pltpu.VMEM((2, 2 if nx > 2 else 1, E, S), f32),
            pltpu.VMEM((2, 2, 2, DOF, S), f32),
            pltpu.VMEM((2, 2, 2, DOF, S), f32),
            pltpu.VMEM((2, 2, 2 * RHS * 8, S), f32),
            pltpu.VMEM((2, 2 * RHS * 8, S), f32),
            pltpu.VMEM((4, DOF, 8, S), f32),
            pltpu.VMEM((nx * nz * nt, 1, 128), f32),
            pltpu.SemaphoreType.DMA,
            pltpu.SemaphoreType.DMA((5,)),
            pltpu.SemaphoreType.DMA((4,)),
            pltpu.SemaphoreType.DMA((2, 4)),
            pltpu.SemaphoreType.DMA,
            pltpu.SemaphoreType.REGULAR,
            pltpu.SemaphoreType.REGULAR,
        ],
        compiler_params=pltpu.CompilerParams(
            collective_id=0, has_side_effects=True, vmem_limit_bytes=56 * 1024 * 1024
        ),
    )(right_side, link_blocks)
    return pl.pallas_call(
        deliver,
        out_shape=(out, out),
        in_specs=[pl.BlockSpec(memory_space=pltpu.VMEM)] * 2,
        out_specs=(pl.BlockSpec(memory_space=pltpu.VMEM),) * 2,
    )(*[pltpu.with_memory_space_constraint(x, pltpu.VMEM) for x in results])


def solution(mesh):
    sizes = tuple(mesh.shape[name] for name in ("xy", "gz", "ta"))
    return jax.shard_map(
        functools.partial(shards, sizes),
        mesh=mesh,
        in_specs=(
            P("xy", "gz", "ta", None, None),
            P("xy", "gz", "ta", None, None, None, None, None),
        ),
        out_specs=(P("xy", "gz", "ta", None, None), P("xy", "gz", "ta", None, None)),
        check_vma=False,
    )
```

```python
import functools
import itertools

import jax
import jax.numpy as jnp
from jax import lax
from jax.experimental import pallas as pl
from jax.experimental.pallas import tpu as pltpu
from jax.sharding import PartitionSpec as P

DOF = 32
RHS = 2
NY = 8
CZ = 2
CT = 8
S = 128
E = 128
MESH = pl.DeviceIdType.MESH

mass_shift = 4.0
epsilon = 1e-06


def cmul(a, b):
    return (a[0] * b[0] - a[1] * b[1], a[0] * b[1] + a[1] * b[0])


def conj(a):
    return (a[0], -a[1])


def cadd(a, b):
    return (a[0] + b[0], a[1] + b[1])


def csub(a, b):
    return (a[0] - b[0], a[1] - b[1])


def scale(a, x):
    return (a[0] * x, a[1] * x)


def size2(a):
    return a[0] * a[0] + a[1] * a[1]


def coefficients(g00, g11, g22, g01, g02, g12):
    beta2 = g00 + epsilon
    beta = jnp.sqrt(beta2)
    inv_beta2 = 1.0 / beta2
    h00 = scale((mass_shift * g00 + g01[0], g01[1]), inv_beta2)
    a = (mass_shift - h00[0], -h00[1])
    left = g11 + size2(a) * g00 + 2.0 * cmul(conj(a), g01)[0]
    h10_2 = jnp.maximum(left, 0.0) * inv_beta2 + epsilon
    h10 = jnp.sqrt(h10_2)
    a4 = (a[0] + mass_shift, a[1])
    a_4 = scale(a, mass_shift)
    top = cadd(cadd(g02, cmul(a4, g01)), scale(a_4, g00))
    h01 = scale(top, inv_beta2 / h10)
    low = cadd(cadd(g12, scale(a4, g11)), cmul(a_4, conj(g01)))
    h11 = scale(cadd(low, cmul(conj(a), top)), inv_beta2 / h10_2)
    p = csub(a4, h11)
    q = csub(csub(a_4, scale(h01, h10)), cmul(h11, a))
    left = g22 + size2(p) * g11 + size2(q) * g00
    left = left + 2.0 * (
        cmul(p, conj(g12))[0] + cmul(q, conj(g02))[0] + cmul(cmul(conj(q), p), g01)[0]
    )
    h21_2 = jnp.maximum(left, 0.0) * (inv_beta2 / h10_2) + epsilon
    m00 = size2(h00) + h10_2
    m01 = cadd(cmul(conj(h00), h01), scale(h11, h10))
    m11 = size2(h01) + size2(h11) + h21_2
    t0 = scale(conj(h00), beta)
    t1 = scale(conj(h01), beta)
    inv_l0 = 1.0 / jnp.sqrt(m00)
    l10 = scale(conj(m01), inv_l0)
    f0 = scale(t0, inv_l0)
    inv_d = 1.0 / (m11 - size2(l10))
    y1 = scale(csub(t1, cmul(l10, f0)), inv_d)
    y0 = scale(csub(f0, cmul(conj(l10), y1)), inv_l0)
    inv_beta = 1.0 / beta
    wb = scale(y1, inv_beta / h10)
    wa = cadd(scale(y0, inv_beta), cmul(wb, a))
    return wa, wb


def kernel(
    sizes, b_hbm, l_hbm, sol_ref, res_ref,
    links, edge_links, z_links, rows, field, kv, turned, xbuf, zbuf, zpack, tbuf, tpack, acc, red,
    b_sem, l_sem, sent, got, got_sum, seen_z, seen_x,
):
    nx, nz, nt = sizes
    total_count = nx * nz * nt
    ix, iz, it = lax.axis_index("xy"), lax.axis_index("gz"), lax.axis_index("ta")
    here = (ix * nz + iz) * nt + it
    groups = DOF // 8
    ways = 2 if nx > 2 else 1

    def step(axis_value, by, count):
        return lax.rem(axis_value + (by + count), count)

    def at(x, z, t):
        return (x, z, t)

    line_x = [at(step(ix, d, nx), iz, it) for d in range(1, nx)]
    line_z = [at(ix, step(iz, d, nz), it) for d in range(1, nz)]
    line_t = [at(ix, iz, step(it, d, nt)) for d in range(1, nt)]

    def tell(sem, devices):
        for device in devices:
            pl.semaphore_signal(sem, inc=1, device_id=device, device_id_type=MESH)

    def remote(source, target, send_sem, recv_sem, device):
        return pltpu.make_async_remote_copy(
            src_ref=source, dst_ref=target, send_sem=send_sem, recv_sem=recv_sem,
            device_id=device, device_id_type=MESH,
        )

    b_copy = pltpu.make_async_copy(b_hbm.at[0, 0, 0], field.at[0], b_sem)
    b_copy.start()

    barrier = pltpu.get_barrier_semaphore()
    tell(barrier, line_t + line_z + line_x)

    for number, k, count in ((0, 0, 1), (0, 3, 2), (1, 7, 2), (1, 5, 2), (2, 1, 2)):
        part = pl.ds(k, count)
        pltpu.make_async_copy(l_hbm.at[0, 0, 0, part], links.at[part], l_sem.at[number]).start(priority=1)

    def wait_links(number, count):
        part = links.at[pl.ds(0, count)]
        pltpu.make_async_copy(part, part, l_sem.at[number]).wait()

    lane = lax.broadcasted_iota(jnp.int32, (8, 128), 1)
    row8 = lax.broadcasted_iota(jnp.int32, (8, 128), 0)
    in_t = lane % CT
    in_z = (lane // CT) % CZ
    odd = lane % 2 == 1

    def rolled(x, by):
        return pltpu.roll(x, by % S, 1) if by % S else x

    def seat(j):
        return (in_t == 2 * j) | (in_t == (2 * j + CT - 1) % CT)

    seats = [seat(j) for j in range(groups)]

    def tiles(ref, first, count):
        return [ref[pl.ds(first + 8 * j, 8), :] for j in range(count)]

    def z_rows(h):
        count = groups // 2
        return [(p, h * count + d, (p * count + d) * 8) for p in range(2) for d in range(count)]

    def halo(n):
        mine = kv.at[n]
        for i in range(2 * RHS):
            rows = tiles(mine, i * DOF, groups)
            packed = None
            for j in range(groups):
                part = jnp.where(odd, rolled(rows[j], 2 * j + CT - 1), rolled(rows[j], 2 * j - CT + 1))
                packed = part if packed is None else jnp.where(seats[j], part, packed)
            tpack[n, pl.ds(8 * i, 8), :] = packed
        for way in (0, 1):
            by = 1 if way else -1
            remote(tpack.at[n], tbuf.at[n, way], sent.at[0], got.at[n, 0], at(ix, iz, step(it, by, nt))).start()
        for h in range(2):
            for p, dj, row in z_rows(h):
                a = mine[pl.ds(p * DOF + 8 * dj, 8), :]
                b = mine[pl.ds((2 + p) * DOF + 8 * dj, 8), :]
                zpack[n, h, 0, pl.ds(row, 8), :] = jnp.where(in_z == 0, a, rolled(b, CT))
                zpack[n, h, 1, pl.ds(row, 8), :] = jnp.where(in_z == 0, rolled(a, -CT), b)
            for way in (0, 1):
                by = 1 if way else -1
                remote(
                    zpack.at[n, h, way], zbuf.at[n, h, way], sent.at[0], got.at[n, 2 + h], at(ix, step(iz, by, nz), it)
                ).start()
        for way in range(ways):
            by = 1 if way else -1
            remote(mine, xbuf.at[n, way], sent.at[0], got.at[n, 1], at(step(ix, by, nx), iz, it)).start()

    def receive(n, kind, ref):
        remote(ref, ref, sent.at[0], got.at[n, kind], (ix, iz, it)).wait_recv()

    def products(passes, fresh, merge=False):
        def block(c0):
            sums = [[None] * (3 * RHS) for _ in range(4)]
            for link, near in passes:
                for j in range(groups):
                    rows = pl.ds(8 * j, 8)
                    vs = []
                    for r in range(RHS):
                        vr = near[pl.ds(2 * r * DOF + 8 * j, 8), :]
                        vi = near[pl.ds((2 * r + 1) * DOF + 8 * j, 8), :]
                        vs += [vr, vi, vr + vi]
                    for q in range(4):
                        c = c0 + q
                        lr = links[link, 0, c, rows, :]
                        li = links[link, 1, c, rows, :]
                        if merge:
                            lr = lr + links[link + 1, 0, c, rows, :]
                            li = li + links[link + 1, 1, c, rows, :]
                            links[link, 0, c, rows, :] = lr
                            links[link, 1, c, rows, :] = li
                        ls = (lr, li, lr + li)
                        for m in range(3 * RHS):
                            x = ls[m % 3] * vs[m]
                            sums[q][m] = x if sums[q][m] is None else sums[q][m] + x
            out = []
            for q in range(4):
                parts = []
                for r in range(RHS):
                    rr, ii, both = sums[q][3 * r : 3 * r + 3]
                    parts += [rr - ii, both - (rr + ii)]
                if not fresh:
                    parts = [acc[i, c0 + q] + parts[i] for i in range(2 * RHS)]
                out.append(parts)
            return out

        def body(step_number, carry):
            c0 = step_number * 4
            out = block(c0)
            for q in range(4):
                for i in range(2 * RHS):
                    acc[i, c0 + q] = out[q][i]
            return carry

        lax.fori_loop(0, DOF // 4, body, 0)

    def split_z():
        def body(c, carry):
            for p in range(2):
                for j in range(groups):
                    rows = pl.ds(8 * j, 8)
                    up, down = links[5, p, c, rows, :], links[6, p, c, rows, :]
                    links[5, p, c, rows, :] = jnp.where(in_z == 0, up, down)
                    z_links[p, pl.ds(c * (DOF + 1) + 8 * j, 8), :] = jnp.where(in_z == 0, down, up)
            return carry

        lax.fori_loop(0, DOF, body, 0, unroll=2)

    def pack_edges():
        last = in_t == CT - 1

        def body(c, carry):
            for p in range(2):
                packed = None
                for j in range(groups):
                    rows = pl.ds(8 * j, 8)
                    part = rolled(jnp.where(last, links[7, p, c, rows, :], links[8, p, c, rows, :]), 2 * j)
                    packed = part if packed is None else jnp.where(seats[j], part, packed)
                edge_links[p, pl.ds(pl.multiple_of(8 * c, 8), 8), :] = packed
            return carry

        lax.fori_loop(0, DOF, body, 0, unroll=8)

    low4, low2, low1 = row8 < 4, row8 % 4 < 2, row8 % 2 < 1

    def fold(xs):
        ys = [
            jnp.where(low4, xs[i], xs[i + 4]) + pltpu.roll(jnp.where(low4, xs[i + 4], xs[i]), 4, 0)
            for i in range(4)
        ]
        zs = [
            jnp.where(low2, ys[i] + pltpu.roll(ys[i], 6, 0), ys[i + 2] + pltpu.roll(ys[i + 2], 2, 0))
            for i in range(2)
        ]
        return jnp.where(low1, zs[0] + pltpu.roll(zs[0], 7, 0), zs[1] + pltpu.roll(zs[1], 1, 0))

    def shift(n):
        mine = kv.at[n]
        for j in range(E // 8):
            rows = pl.ds(8 * j, 8)
            own = mine[rows, :]
            turned[0, rows, :] = rolled(own, -CZ * CT)
            turned[1, rows, :] = rolled(own, CZ * CT)
            turned[2, rows, :] = jnp.where(in_z == 0, rolled(own, -CT), rolled(own, CT))
            turned[3, rows, :] = jnp.where(in_t == CT - 1, 0.0, rolled(own, -1))
            turned[4, rows, :] = jnp.where(in_t == 0, 0.0, rolled(own, 1))

    def row_products(link_at, row_at, steps):
        sums = [[None] * groups for _ in range(3 * RHS)]
        for d in steps:
            vs = [jnp.broadcast_to(row_at(m, d), (8, 128)) for m in range(3 * RHS)]
            for g in range(groups):
                lr, li = link_at(0, g, d), link_at(1, g, d)
                ls = (lr, li, lr + li)
                for m in range(3 * RHS):
                    x = ls[m % 3] * vs[m]
                    sums[m][g] = x if sums[m][g] is None else sums[m][g] + x
        out = []
        for r in range(RHS):
            rr, ii, both = sums[3 * r : 3 * r + 3]
            out.append([rr[g] - ii[g] for g in range(groups)])
            out.append([both[g] - (rr[g] + ii[g]) for g in range(groups)])
        return out

    local = ((0, None), (3, 0), (4, 1), (7, 3), (8, 4), (5, 2))

    def apply(n):
        shift(n)
        terms = [(link, kv.at[n] if near is None else turned.at[near]) for link, near in local]
        if n == 0:
            wait_links(0, 3)
            products(terms[:3], True)
            wait_links(1, 4)
            products(terms[3:5], False)
            pack_edges()
            split_z()
            products(terms[5:], False)
            pl.semaphore_wait(seen_z, len(line_z))
            tell(seen_x, line_x)
            wait_links(2, 2)
        else:
            products(terms, True)
            early()
        receive(n, 1, xbuf.at[n, pl.ds(0, ways)])
        if nx > 2:
            products(((1, xbuf.at[n, 0]), (2, xbuf.at[n, 1])), False)
        else:
            products(((1, xbuf.at[n, 0]),), False, n == 0)
        for i in range(4):
            for c in range(0, DOF, 8):
                turned[0, pl.ds(i * DOF + c, 8), :] = fold([acc[i, c + j] for j in range(8)])
        for h in range(2):
            receive(n, 2 + h, zbuf.at[n, h])
            near = {}
            for p, dj, row in z_rows(h):
                p0 = zbuf[n, h, 0, pl.ds(row, 8), :]
                p1 = zbuf[n, h, 1, pl.ds(row, 8), :]
                near[0, p, dj] = jnp.where(in_z == 0, p1, rolled(p0, CT))
                near[1, p, dj] = jnp.where(in_z == 0, rolled(p1, -CT), p0)
            for r, p, dj in near:
                rows[3 * r + p, pl.ds(8 * dj, 8), :] = near[r, p, dj]
                if p == 0:
                    rows[3 * r + 2, pl.ds(8 * dj, 8), :] = near[r, 0, dj] + near[r, 1, dj]
            got_z = row_products(
                lambda p, g, d: z_links[p, pl.ds(8 * g * (DOF + 1) + d, 8, stride=DOF + 1), :],
                lambda m, d: rows[m, pl.ds(d, 1), :],
                range(h * DOF // 2, (h + 1) * DOF // 2),
            )
            for i in range(4):
                for g in range(groups):
                    place = pl.ds(i * DOF + 8 * g, 8)
                    turned[0, place, :] = turned[0, place, :] + got_z[i][g]
        receive(n, 0, tbuf.at[n])
        for r in range(RHS):
            vr, vi = (
                jnp.where(odd, tbuf[n, 0, pl.ds(8 * i, 8), :], tbuf[n, 1, pl.ds(8 * i, 8), :])
                for i in (2 * r, 2 * r + 1)
            )
            for m, v in enumerate((vr, vi, vr + vi)):
                rows[3 * r + m, pl.ds(DOF, 8), :] = v
        got_t = row_products(
            lambda p, g, d: edge_links[p, pl.ds(64 * g + d, 8, stride=8), :],
            lambda m, d: rows[m, pl.ds(DOF + d, 1), :],
            range(8),
        )
        for i in range(4):
            for g in range(groups):
                d = got_t[i][g]
                d = (d + rolled(d, -2)) + (rolled(d, -4) + rolled(d, -6))
                place = pl.ds(i * DOF + 8 * g, 8)
                kv[n + 1, place, :] = turned[0, place, :] + jnp.where(seats[0], d, 0.0)

    def dots(a, b, both):
        out = []
        for r in range(RHS):
            re = im = None
            for j in range(groups):
                ar, ai = (a[pl.ds((2 * r + p) * DOF + 8 * j, 8), :] for p in range(2))
                br, bi = (b[pl.ds((2 * r + p) * DOF + 8 * j, 8), :] for p in range(2))
                x = ar * br + ai * bi
                re = x if re is None else re + x
                if both:
                    x = ar * bi - ai * br
                    im = x if im is None else im + x
            out.append((re, im) if both else (re,))
        return out

    def lane_sums(x):
        return jnp.broadcast_to(jnp.sum(x, axis=1, keepdims=True), (8, 128))

    def early():
        d00, d11, d01 = dots(kv.at[0], kv.at[0], False), dots(kv.at[1], kv.at[1], False), dots(kv.at[0], kv.at[1], True)
        sums = lane_sums(fold([x for r in range(RHS) for x in d00[r] + d11[r] + d01[r]]))
        acc_row = jnp.where(lane == row8, sums, 0.0)
        field[4, pl.ds(0, 8), :] = acc_row

    b_copy.wait()
    kv[0] = field[0].T
    pl.semaphore_wait(barrier, len(line_t) + len(line_z) + len(line_x))
    halo(0)
    tell(seen_z, line_z)
    apply(0)
    halo(1)
    apply(1)

    d02, d12, d22 = dots(kv.at[0], kv.at[2], True), dots(kv.at[1], kv.at[2], True), dots(kv.at[2], kv.at[2], False)
    sums = lane_sums(fold([x for r in range(RHS) for x in d02[r] + d12[r]]))
    a, b = d22[0][0], d22[1][0]
    norms = lane_sums(jnp.where(low4, a + pltpu.roll(a, 4, 0), b + pltpu.roll(b, 4, 0)))
    mine = field[4, pl.ds(0, 8), :] + jnp.where(lane == 8 + row8, sums, 0.0)
    mine = mine + jnp.where(lane == 16 + row8 // 4, norms, 0.0)
    pl.semaphore_wait(seen_x, len(line_x))
    red[here] = jnp.sum(mine, axis=0, keepdims=True)
    for x, z, t in itertools.product(range(nx), range(nz), range(nt)):

        @pl.when((x * nz + z) * nt + t != here)
        def _():
            remote(red.at[here], red.at[here], sent.at[1], got_sum, (x, z, t)).start()

    in_p = (lax.broadcasted_iota(jnp.int32, (S, E), 1) // DOF) % 2

    def aside(v):
        return jnp.where(in_p == 0, pltpu.roll(v, E - DOF, 1), -pltpu.roll(v, DOF, 1))

    k0, k1, k2 = field[0], kv[1].T, kv[2].T
    low, high = mass_shift * k0 + k1, mass_shift * k1 + k2
    for number, v in enumerate((k0, k1, low, high)):
        if number:
            field[number] = v
        turned[number] = aside(v)
    halo_bytes = links.at[0, 0, pl.ds(0, 2 * (2 + 4 + ways * E // DOF))]
    remote(halo_bytes, halo_bytes, sent.at[0], got_sum, (ix, iz, it)).wait_send()

    others = red.at[pl.ds(0, total_count - 1)]
    remote(others, others, sent.at[1], got_sum, (ix, iz, it)).wait_recv()
    value = jnp.broadcast_to(jnp.sum(red[...], axis=0), (8, 128))
    first_half = lane < 2 * DOF

    def pick(place):
        return [jnp.sum(jnp.where(lane == place + by * r, value, 0.0), axis=1, keepdims=True) for r, by in ((0, 0), (1, 4))]

    place = (row8 // 4) * 8 + row8 % 4
    low, high = pick(place)
    gram = jnp.where(first_half, low, high)
    low, _ = pick(16 + row8 * 0)
    high, _ = pick(17 + row8 * 0)
    g22 = jnp.where(first_half, low, high)[0:1]
    g = [gram[i : i + 1] for i in range(8)]
    wa, wb = coefficients(g[0], g[1], g22, (g[2], g[3]), (g[4], g[5]), (g[6], g[7]))

    wa, wb = ([jnp.broadcast_to(x, (8, 128)) for x in w] for w in (wa, wb))
    for j in range(S // 8):
        rows8 = pl.ds(8 * j, 8)
        k0, k1, low, high = (field[number, rows8, :] for number in range(4))
        z0, z1, z_low, z_high = (turned[number, rows8, :] for number in range(4))
        sol_ref[0, 0, 0, rows8, :] = (wa[0] * k0 - wa[1] * z0) + (wb[0] * k1 - wb[1] * z1)
        res_ref[0, 0, 0, rows8, :] = k0 - (wa[0] * low - wa[1] * z_low) - (wb[0] * high - wb[1] * z_high)
    remote(others, others, sent.at[1], got_sum, (ix, iz, it)).wait_send()


def deliver(a_ref, b_ref, sol_ref, res_ref):
    sol_ref[...] = a_ref[...]
    res_ref[...] = b_ref[...]


def shards(sizes, right_side, link_blocks):
    nx, nz, nt = sizes
    out = jax.ShapeDtypeStruct(right_side.shape, jnp.float32)
    f32 = jnp.float32
    held = pltpu.VMEM(right_side.shape, f32)
    results = pl.pallas_call(
        functools.partial(kernel, sizes),
        out_shape=(held, held),
        in_specs=[pl.BlockSpec(memory_space=pl.ANY)] * 2,
        out_specs=(pl.BlockSpec(memory_space=pltpu.VMEM),) * 2,
        scratch_shapes=[
            pltpu.VMEM((9, 2, DOF, DOF, S), f32),
            pltpu.VMEM((2, DOF * 8, S), f32),
            pltpu.VMEM((2, DOF * (DOF + 1), S), f32),
            pltpu.VMEM((3 * RHS, DOF + 8, S), f32),
            pltpu.VMEM((5, S, E), f32),
            pltpu.VMEM((3, E, S), f32),
            pltpu.VMEM((5, E, S), f32),
            pltpu.VMEM((2, 2 if nx > 2 else 1, E, S), f32),
            pltpu.VMEM((2, 2, 2, DOF, S), f32),
            pltpu.VMEM((2, 2, 2, DOF, S), f32),
            pltpu.VMEM((2, 2, 2 * RHS * 8, S), f32),
            pltpu.VMEM((2, 2 * RHS * 8, S), f32),
            pltpu.VMEM((4, DOF, 8, S), f32),
            pltpu.VMEM((nx * nz * nt, 1, 128), f32),
            pltpu.SemaphoreType.DMA,
            pltpu.SemaphoreType.DMA((3,)),
            pltpu.SemaphoreType.DMA((2,)),
            pltpu.SemaphoreType.DMA((2, 4)),
            pltpu.SemaphoreType.DMA,
            pltpu.SemaphoreType.REGULAR,
            pltpu.SemaphoreType.REGULAR,
        ],
        compiler_params=pltpu.CompilerParams(
            collective_id=0, has_side_effects=True, vmem_limit_bytes=56 * 1024 * 1024
        ),
    )(right_side, link_blocks)
    return pl.pallas_call(
        deliver,
        out_shape=(out, out),
        in_specs=[pl.BlockSpec(memory_space=pltpu.VMEM)] * 2,
        out_specs=(pl.BlockSpec(memory_space=pltpu.VMEM),) * 2,
    )(*[pltpu.with_memory_space_constraint(x, pltpu.VMEM) for x in results])


def solution(mesh):
    sizes = tuple(mesh.shape[name] for name in ("xy", "gz", "ta"))
    return jax.shard_map(
        functools.partial(shards, sizes),
        mesh=mesh,
        in_specs=(
            P("xy", "gz", "ta", None, None),
            P("xy", "gz", "ta", None, None, None, None, None),
        ),
        out_specs=(P("xy", "gz", "ta", None, None), P("xy", "gz", "ta", None, None)),
        check_vma=False,
    )
```

```python
import functools
import itertools

import jax
import jax.numpy as jnp
from jax import lax
from jax.experimental import pallas as pl
from jax.experimental.pallas import tpu as pltpu
from jax.sharding import PartitionSpec as P

DOF = 32
RHS = 2
NY = 8
CZ = 2
CT = 8
S = 128
E = 128
MESH = pl.DeviceIdType.MESH

mass_shift = 4.0
epsilon = 1e-06


def cmul(a, b):
    return (a[0] * b[0] - a[1] * b[1], a[0] * b[1] + a[1] * b[0])


def conj(a):
    return (a[0], -a[1])


def cadd(a, b):
    return (a[0] + b[0], a[1] + b[1])


def csub(a, b):
    return (a[0] - b[0], a[1] - b[1])


def scale(a, x):
    return (a[0] * x, a[1] * x)


def size2(a):
    return a[0] * a[0] + a[1] * a[1]


def coefficients(g00, g11, g22, g01, g02, g12):
    beta2 = g00 + epsilon
    beta = jnp.sqrt(beta2)
    inv_beta2 = 1.0 / beta2
    h00 = scale((mass_shift * g00 + g01[0], g01[1]), inv_beta2)
    a = (mass_shift - h00[0], -h00[1])
    left = g11 + size2(a) * g00 + 2.0 * cmul(conj(a), g01)[0]
    h10_2 = jnp.maximum(left, 0.0) * inv_beta2 + epsilon
    h10 = jnp.sqrt(h10_2)
    a4 = (a[0] + mass_shift, a[1])
    a_4 = scale(a, mass_shift)
    top = cadd(cadd(g02, cmul(a4, g01)), scale(a_4, g00))
    h01 = scale(top, inv_beta2 / h10)
    low = cadd(cadd(g12, scale(a4, g11)), cmul(a_4, conj(g01)))
    h11 = scale(cadd(low, cmul(conj(a), top)), inv_beta2 / h10_2)
    p = csub(a4, h11)
    q = csub(csub(a_4, scale(h01, h10)), cmul(h11, a))
    left = g22 + size2(p) * g11 + size2(q) * g00
    left = left + 2.0 * (
        cmul(p, conj(g12))[0] + cmul(q, conj(g02))[0] + cmul(cmul(conj(q), p), g01)[0]
    )
    h21_2 = jnp.maximum(left, 0.0) * (inv_beta2 / h10_2) + epsilon
    m00 = size2(h00) + h10_2
    m01 = cadd(cmul(conj(h00), h01), scale(h11, h10))
    m11 = size2(h01) + size2(h11) + h21_2
    t0 = scale(conj(h00), beta)
    t1 = scale(conj(h01), beta)
    inv_l0 = 1.0 / jnp.sqrt(m00)
    l10 = scale(conj(m01), inv_l0)
    f0 = scale(t0, inv_l0)
    inv_d = 1.0 / (m11 - size2(l10))
    y1 = scale(csub(t1, cmul(l10, f0)), inv_d)
    y0 = scale(csub(f0, cmul(conj(l10), y1)), inv_l0)
    inv_beta = 1.0 / beta
    wb = scale(y1, inv_beta / h10)
    wa = cadd(scale(y0, inv_beta), cmul(wb, a))
    return wa, wb


def kernel(
    sizes, b_hbm, l_hbm, sol_ref, res_ref,
    links, edge_links, z_links, rows, field, kv, turned, xbuf, zbuf, zpack, tbuf, tpack, acc, red,
    b_sem, l_sem, sent, got, got_sum, seen_z, seen_x,
):
    nx, nz, nt = sizes
    total_count = nx * nz * nt
    ix, iz, it = lax.axis_index("xy"), lax.axis_index("gz"), lax.axis_index("ta")
    here = (ix * nz + iz) * nt + it
    groups = DOF // 8
    ways = 2 if nx > 2 else 1

    def step(axis_value, by, count):
        return lax.rem(axis_value + (by + count), count)

    def at(x, z, t):
        return (x, z, t)

    line_x = [at(step(ix, d, nx), iz, it) for d in range(1, nx)]
    line_z = [at(ix, step(iz, d, nz), it) for d in range(1, nz)]
    line_t = [at(ix, iz, step(it, d, nt)) for d in range(1, nt)]

    def tell(sem, devices):
        for device in devices:
            pl.semaphore_signal(sem, inc=1, device_id=device, device_id_type=MESH)

    def remote(source, target, send_sem, recv_sem, device):
        return pltpu.make_async_remote_copy(
            src_ref=source, dst_ref=target, send_sem=send_sem, recv_sem=recv_sem,
            device_id=device, device_id_type=MESH,
        )

    b_copy = pltpu.make_async_copy(b_hbm.at[0, 0, 0], field.at[0], b_sem)
    b_copy.start()

    barrier = pltpu.get_barrier_semaphore()
    tell(barrier, line_t + line_z + line_x)

    for number, k, count in ((0, 7, 2), (1, 5, 2), (1, 0, 1), (2, 3, 2), (3, 1, 2)):
        part = pl.ds(k, count)
        pltpu.make_async_copy(l_hbm.at[0, 0, 0, part], links.at[part], l_sem.at[number]).start(priority=1)

    def wait_links(number, count):
        part = links.at[pl.ds(0, count)]
        pltpu.make_async_copy(part, part, l_sem.at[number]).wait()

    lane = lax.broadcasted_iota(jnp.int32, (8, 128), 1)
    row8 = lax.broadcasted_iota(jnp.int32, (8, 128), 0)
    in_t = lane % CT
    in_z = (lane // CT) % CZ
    odd = lane % 2 == 1

    def rolled(x, by):
        return pltpu.roll(x, by % S, 1) if by % S else x

    def seat(j):
        return (in_t == 2 * j) | (in_t == (2 * j + CT - 1) % CT)

    seats = [seat(j) for j in range(groups)]

    def tiles(ref, first, count):
        return [ref[pl.ds(first + 8 * j, 8), :] for j in range(count)]

    def z_rows(h):
        count = groups // 2
        return [(p, h * count + d, (p * count + d) * 8) for p in range(2) for d in range(count)]

    def halo(n):
        mine = kv.at[n]
        for i in range(2 * RHS):
            rows = tiles(mine, i * DOF, groups)
            packed = None
            for j in range(groups):
                part = jnp.where(odd, rolled(rows[j], 2 * j + CT - 1), rolled(rows[j], 2 * j - CT + 1))
                packed = part if packed is None else jnp.where(seats[j], part, packed)
            tpack[n, pl.ds(8 * i, 8), :] = packed
        for way in (0, 1):
            by = 1 if way else -1
            remote(tpack.at[n], tbuf.at[n, way], sent.at[0], got.at[n, 0], at(ix, iz, step(it, by, nt))).start()
        for h in range(2):
            for p, dj, row in z_rows(h):
                a = mine[pl.ds(p * DOF + 8 * dj, 8), :]
                b = mine[pl.ds((2 + p) * DOF + 8 * dj, 8), :]
                zpack[n, h, 0, pl.ds(row, 8), :] = jnp.where(in_z == 0, a, rolled(b, CT))
                zpack[n, h, 1, pl.ds(row, 8), :] = jnp.where(in_z == 0, rolled(a, -CT), b)
            for way in (0, 1):
                by = 1 if way else -1
                remote(
                    zpack.at[n, h, way], zbuf.at[n, h, way], sent.at[0], got.at[n, 2 + h], at(ix, step(iz, by, nz), it)
                ).start()
        for way in range(ways):
            by = 1 if way else -1
            remote(mine, xbuf.at[n, way], sent.at[0], got.at[n, 1], at(step(ix, by, nx), iz, it)).start()

    def receive(n, kind, ref):
        remote(ref, ref, sent.at[0], got.at[n, kind], (ix, iz, it)).wait_recv()

    def products(passes, fresh, merge=False):
        def block(c0):
            sums = [[None] * (3 * RHS) for _ in range(4)]
            for link, near in passes:
                for j in range(groups):
                    rows = pl.ds(8 * j, 8)
                    vs = []
                    for r in range(RHS):
                        vr = near[pl.ds(2 * r * DOF + 8 * j, 8), :]
                        vi = near[pl.ds((2 * r + 1) * DOF + 8 * j, 8), :]
                        vs += [vr, vi, vr + vi]
                    for q in range(4):
                        c = c0 + q
                        lr = links[link, 0, c, rows, :]
                        li = links[link, 1, c, rows, :]
                        if merge:
                            lr = lr + links[link + 1, 0, c, rows, :]
                            li = li + links[link + 1, 1, c, rows, :]
                            links[link, 0, c, rows, :] = lr
                            links[link, 1, c, rows, :] = li
                        ls = (lr, li, lr + li)
                        for m in range(3 * RHS):
                            x = ls[m % 3] * vs[m]
                            sums[q][m] = x if sums[q][m] is None else sums[q][m] + x
            out = []
            for q in range(4):
                parts = []
                for r in range(RHS):
                    rr, ii, both = sums[q][3 * r : 3 * r + 3]
                    parts += [rr - ii, both - (rr + ii)]
                if not fresh:
                    parts = [acc[i, c0 + q] + parts[i] for i in range(2 * RHS)]
                out.append(parts)
            return out

        def body(step_number, carry):
            c0 = step_number * 4
            out = block(c0)
            for q in range(4):
                for i in range(2 * RHS):
                    acc[i, c0 + q] = out[q][i]
            return carry

        lax.fori_loop(0, DOF // 4, body, 0)

    def split_z():
        def body(c, carry):
            for p in range(2):
                for j in range(groups):
                    rows = pl.ds(8 * j, 8)
                    up, down = links[5, p, c, rows, :], links[6, p, c, rows, :]
                    links[5, p, c, rows, :] = jnp.where(in_z == 0, up, down)
                    z_links[p, pl.ds(c * (DOF + 1) + 8 * j, 8), :] = jnp.where(in_z == 0, down, up)
            return carry

        lax.fori_loop(0, DOF, body, 0, unroll=2)

    def pack_edges():
        last = in_t == CT - 1

        def body(c, carry):
            for p in range(2):
                packed = None
                for j in range(groups):
                    rows = pl.ds(8 * j, 8)
                    part = rolled(jnp.where(last, links[7, p, c, rows, :], links[8, p, c, rows, :]), 2 * j)
                    packed = part if packed is None else jnp.where(seats[j], part, packed)
                edge_links[p, pl.ds(pl.multiple_of(8 * c, 8), 8), :] = packed
            return carry

        lax.fori_loop(0, DOF, body, 0, unroll=8)

    low4, low2, low1 = row8 < 4, row8 % 4 < 2, row8 % 2 < 1

    def fold(xs):
        ys = [
            jnp.where(low4, xs[i], xs[i + 4]) + pltpu.roll(jnp.where(low4, xs[i + 4], xs[i]), 4, 0)
            for i in range(4)
        ]
        zs = [
            jnp.where(low2, ys[i] + pltpu.roll(ys[i], 6, 0), ys[i + 2] + pltpu.roll(ys[i + 2], 2, 0))
            for i in range(2)
        ]
        return jnp.where(low1, zs[0] + pltpu.roll(zs[0], 7, 0), zs[1] + pltpu.roll(zs[1], 1, 0))

    def shift(n):
        mine = kv.at[n]
        for j in range(E // 8):
            rows = pl.ds(8 * j, 8)
            own = mine[rows, :]
            turned[0, rows, :] = rolled(own, -CZ * CT)
            turned[1, rows, :] = rolled(own, CZ * CT)
            turned[2, rows, :] = jnp.where(in_z == 0, rolled(own, -CT), rolled(own, CT))
            turned[3, rows, :] = jnp.where(in_t == CT - 1, 0.0, rolled(own, -1))
            turned[4, rows, :] = jnp.where(in_t == 0, 0.0, rolled(own, 1))

    def row_products(link_at, row_at, steps):
        sums = [[None] * groups for _ in range(3 * RHS)]
        for d in steps:
            vs = [jnp.broadcast_to(row_at(m, d), (8, 128)) for m in range(3 * RHS)]
            for g in range(groups):
                lr, li = link_at(0, g, d), link_at(1, g, d)
                ls = (lr, li, lr + li)
                for m in range(3 * RHS):
                    x = ls[m % 3] * vs[m]
                    sums[m][g] = x if sums[m][g] is None else sums[m][g] + x
        out = []
        for r in range(RHS):
            rr, ii, both = sums[3 * r : 3 * r + 3]
            out.append([rr[g] - ii[g] for g in range(groups)])
            out.append([both[g] - (rr[g] + ii[g]) for g in range(groups)])
        return out

    local = ((7, 3), (8, 4), (5, 2), (0, None), (3, 0), (4, 1))

    def near_of(n, terms):
        return [(link, kv.at[n] if near is None else turned.at[near]) for link, near in terms]

    def local_first():
        wait_links(0, 2)
        products(near_of(0, local[:2]), True)
        pack_edges()
        wait_links(1, 3)
        split_z()
        products(near_of(0, local[2:4]), False)

    def apply(n):
        if n == 0:

            @pl.when(it != 0)
            def _():
                shift(0)
                local_first()

            wait_links(2, 2)
            products(near_of(0, local[4:]), False)
            pl.semaphore_wait(seen_z, len(line_z))
            tell(seen_x, line_x)
            wait_links(3, 2)
        else:
            shift(1)
            products(near_of(1, local), True)
            early()
        receive(n, 1, xbuf.at[n, pl.ds(0, ways)])
        if nx > 2:
            products(((1, xbuf.at[n, 0]), (2, xbuf.at[n, 1])), False)
        else:
            products(((1, xbuf.at[n, 0]),), False, n == 0)
        for i in range(4):
            for c in range(0, DOF, 8):
                turned[0, pl.ds(i * DOF + c, 8), :] = fold([acc[i, c + j] for j in range(8)])
        for h in range(2):
            receive(n, 2 + h, zbuf.at[n, h])
            near = {}
            for p, dj, row in z_rows(h):
                p0 = zbuf[n, h, 0, pl.ds(row, 8), :]
                p1 = zbuf[n, h, 1, pl.ds(row, 8), :]
                near[0, p, dj] = jnp.where(in_z == 0, p1, rolled(p0, CT))
                near[1, p, dj] = jnp.where(in_z == 0, rolled(p1, -CT), p0)
            for r, p, dj in near:
                rows[3 * r + p, pl.ds(8 * dj, 8), :] = near[r, p, dj]
                if p == 0:
                    rows[3 * r + 2, pl.ds(8 * dj, 8), :] = near[r, 0, dj] + near[r, 1, dj]
            got_z = row_products(
                lambda p, g, d: z_links[p, pl.ds(8 * g * (DOF + 1) + d, 8, stride=DOF + 1), :],
                lambda m, d: rows[m, pl.ds(d, 1), :],
                range(h * DOF // 2, (h + 1) * DOF // 2),
            )
            for i in range(4):
                for g in range(groups):
                    place = pl.ds(i * DOF + 8 * g, 8)
                    turned[0, place, :] = turned[0, place, :] + got_z[i][g]
        receive(n, 0, tbuf.at[n])
        for r in range(RHS):
            vr, vi = (
                jnp.where(odd, tbuf[n, 0, pl.ds(8 * i, 8), :], tbuf[n, 1, pl.ds(8 * i, 8), :])
                for i in (2 * r, 2 * r + 1)
            )
            for m, v in enumerate((vr, vi, vr + vi)):
                rows[3 * r + m, pl.ds(DOF, 8), :] = v
        got_t = row_products(
            lambda p, g, d: edge_links[p, pl.ds(64 * g + d, 8, stride=8), :],
            lambda m, d: rows[m, pl.ds(DOF + d, 1), :],
            range(8),
        )
        for i in range(4):
            for g in range(groups):
                d = got_t[i][g]
                d = (d + rolled(d, -2)) + (rolled(d, -4) + rolled(d, -6))
                place = pl.ds(i * DOF + 8 * g, 8)
                kv[n + 1, place, :] = turned[0, place, :] + jnp.where(seats[0], d, 0.0)

    def dots(a, b, both):
        out = []
        for r in range(RHS):
            re = im = None
            for j in range(groups):
                ar, ai = (a[pl.ds((2 * r + p) * DOF + 8 * j, 8), :] for p in range(2))
                br, bi = (b[pl.ds((2 * r + p) * DOF + 8 * j, 8), :] for p in range(2))
                x = ar * br + ai * bi
                re = x if re is None else re + x
                if both:
                    x = ar * bi - ai * br
                    im = x if im is None else im + x
            out.append((re, im) if both else (re,))
        return out

    def lane_sums(x):
        return jnp.broadcast_to(jnp.sum(x, axis=1, keepdims=True), (8, 128))

    def early():
        d00, d11, d01 = dots(kv.at[0], kv.at[0], False), dots(kv.at[1], kv.at[1], False), dots(kv.at[0], kv.at[1], True)
        sums = lane_sums(fold([x for r in range(RHS) for x in d00[r] + d11[r] + d01[r]]))
        acc_row = jnp.where(lane == row8, sums, 0.0)
        field[4, pl.ds(0, 8), :] = acc_row

    b_copy.wait()
    kv[0] = field[0].T

    @pl.when(it == 0)
    def _():
        shift(0)
        local_first()

    pl.semaphore_wait(barrier, len(line_t) + len(line_z) + len(line_x))
    halo(0)
    tell(seen_z, line_z)
    apply(0)
    halo(1)
    apply(1)

    d02, d12, d22 = dots(kv.at[0], kv.at[2], True), dots(kv.at[1], kv.at[2], True), dots(kv.at[2], kv.at[2], False)
    sums = lane_sums(fold([x for r in range(RHS) for x in d02[r] + d12[r]]))
    a, b = d22[0][0], d22[1][0]
    norms = lane_sums(jnp.where(low4, a + pltpu.roll(a, 4, 0), b + pltpu.roll(b, 4, 0)))
    mine = field[4, pl.ds(0, 8), :] + jnp.where(lane == 8 + row8, sums, 0.0)
    mine = mine + jnp.where(lane == 16 + row8 // 4, norms, 0.0)
    pl.semaphore_wait(seen_x, len(line_x))
    red[here] = jnp.sum(mine, axis=0, keepdims=True)
    for x, z, t in itertools.product(range(nx), range(nz), range(nt)):

        @pl.when((x * nz + z) * nt + t != here)
        def _():
            remote(red.at[here], red.at[here], sent.at[1], got_sum, (x, z, t)).start()

    in_p = (lax.broadcasted_iota(jnp.int32, (S, E), 1) // DOF) % 2

    def aside(v):
        return jnp.where(in_p == 0, pltpu.roll(v, E - DOF, 1), -pltpu.roll(v, DOF, 1))

    k0, k1, k2 = field[0], kv[1].T, kv[2].T
    low, high = mass_shift * k0 + k1, mass_shift * k1 + k2
    for number, v in enumerate((k0, k1, low, high)):
        if number:
            field[number] = v
        turned[number] = aside(v)
    halo_bytes = links.at[0, 0, pl.ds(0, 2 * (2 + 4 + ways * E // DOF))]
    remote(halo_bytes, halo_bytes, sent.at[0], got_sum, (ix, iz, it)).wait_send()

    others = red.at[pl.ds(0, total_count - 1)]
    remote(others, others, sent.at[1], got_sum, (ix, iz, it)).wait_recv()
    value = jnp.broadcast_to(jnp.sum(red[...], axis=0), (8, 128))
    first_half = lane < 2 * DOF

    def pick(place):
        return [jnp.sum(jnp.where(lane == place + by * r, value, 0.0), axis=1, keepdims=True) for r, by in ((0, 0), (1, 4))]

    place = (row8 // 4) * 8 + row8 % 4
    low, high = pick(place)
    gram = jnp.where(first_half, low, high)
    low, _ = pick(16 + row8 * 0)
    high, _ = pick(17 + row8 * 0)
    g22 = jnp.where(first_half, low, high)[0:1]
    g = [gram[i : i + 1] for i in range(8)]
    wa, wb = coefficients(g[0], g[1], g22, (g[2], g[3]), (g[4], g[5]), (g[6], g[7]))

    wa, wb = ([jnp.broadcast_to(x, (8, 128)) for x in w] for w in (wa, wb))
    for j in range(S // 8):
        rows8 = pl.ds(8 * j, 8)
        k0, k1, low, high = (field[number, rows8, :] for number in range(4))
        z0, z1, z_low, z_high = (turned[number, rows8, :] for number in range(4))
        sol_ref[0, 0, 0, rows8, :] = (wa[0] * k0 - wa[1] * z0) + (wb[0] * k1 - wb[1] * z1)
        res_ref[0, 0, 0, rows8, :] = k0 - (wa[0] * low - wa[1] * z_low) - (wb[0] * high - wb[1] * z_high)
    remote(others, others, sent.at[1], got_sum, (ix, iz, it)).wait_send()


def deliver(a_ref, b_ref, sol_ref, res_ref):
    sol_ref[...] = a_ref[...]
    res_ref[...] = b_ref[...]


def shards(sizes, right_side, link_blocks):
    nx, nz, nt = sizes
    out = jax.ShapeDtypeStruct(right_side.shape, jnp.float32)
    f32 = jnp.float32
    held = pltpu.VMEM(right_side.shape, f32)
    results = pl.pallas_call(
        functools.partial(kernel, sizes),
        out_shape=(held, held),
        in_specs=[pl.BlockSpec(memory_space=pl.ANY)] * 2,
        out_specs=(pl.BlockSpec(memory_space=pltpu.VMEM),) * 2,
        scratch_shapes=[
            pltpu.VMEM((9, 2, DOF, DOF, S), f32),
            pltpu.VMEM((2, DOF * 8, S), f32),
            pltpu.VMEM((2, DOF * (DOF + 1), S), f32),
            pltpu.VMEM((3 * RHS, DOF + 8, S), f32),
            pltpu.VMEM((5, S, E), f32),
            pltpu.VMEM((3, E, S), f32),
            pltpu.VMEM((5, E, S), f32),
            pltpu.VMEM((2, 2 if nx > 2 else 1, E, S), f32),
            pltpu.VMEM((2, 2, 2, DOF, S), f32),
            pltpu.VMEM((2, 2, 2, DOF, S), f32),
            pltpu.VMEM((2, 2, 2 * RHS * 8, S), f32),
            pltpu.VMEM((2, 2 * RHS * 8, S), f32),
            pltpu.VMEM((4, DOF, 8, S), f32),
            pltpu.VMEM((nx * nz * nt, 1, 128), f32),
            pltpu.SemaphoreType.DMA,
            pltpu.SemaphoreType.DMA((4,)),
            pltpu.SemaphoreType.DMA((2,)),
            pltpu.SemaphoreType.DMA((2, 4)),
            pltpu.SemaphoreType.DMA,
            pltpu.SemaphoreType.REGULAR,
            pltpu.SemaphoreType.REGULAR,
        ],
        compiler_params=pltpu.CompilerParams(
            collective_id=0, has_side_effects=True, vmem_limit_bytes=56 * 1024 * 1024
        ),
    )(right_side, link_blocks)
    return pl.pallas_call(
        deliver,
        out_shape=(out, out),
        in_specs=[pl.BlockSpec(memory_space=pltpu.VMEM)] * 2,
        out_specs=(pl.BlockSpec(memory_space=pltpu.VMEM),) * 2,
    )(*[pltpu.with_memory_space_constraint(x, pltpu.VMEM) for x in results])


def solution(mesh):
    sizes = tuple(mesh.shape[name] for name in ("xy", "gz", "ta"))
    return jax.shard_map(
        functools.partial(shards, sizes),
        mesh=mesh,
        in_specs=(
            P("xy", "gz", "ta", None, None),
            P("xy", "gz", "ta", None, None, None, None, None),
        ),
        out_specs=(P("xy", "gz", "ta", None, None), P("xy", "gz", "ta", None, None)),
        check_vma=False,
    )
```

```python
import functools
import itertools

import jax
import jax.numpy as jnp
from jax import lax
from jax.experimental import pallas as pl
from jax.experimental.pallas import tpu as pltpu
from jax.sharding import PartitionSpec as P

DOF = 32
RHS = 2
NY = 8
CZ = 2
CT = 8
S = 128
E = 128
MESH = pl.DeviceIdType.MESH

mass_shift = 4.0
epsilon = 1e-06


def cmul(a, b):
    return (a[0] * b[0] - a[1] * b[1], a[0] * b[1] + a[1] * b[0])


def conj(a):
    return (a[0], -a[1])


def cadd(a, b):
    return (a[0] + b[0], a[1] + b[1])


def csub(a, b):
    return (a[0] - b[0], a[1] - b[1])


def scale(a, x):
    return (a[0] * x, a[1] * x)


def size2(a):
    return a[0] * a[0] + a[1] * a[1]


def coefficients(g00, g11, g22, g01, g02, g12):
    beta2 = g00 + epsilon
    beta = jnp.sqrt(beta2)
    inv_beta2 = 1.0 / beta2
    h00 = scale((mass_shift * g00 + g01[0], g01[1]), inv_beta2)
    a = (mass_shift - h00[0], -h00[1])
    left = g11 + size2(a) * g00 + 2.0 * cmul(conj(a), g01)[0]
    h10_2 = jnp.maximum(left, 0.0) * inv_beta2 + epsilon
    h10 = jnp.sqrt(h10_2)
    a4 = (a[0] + mass_shift, a[1])
    a_4 = scale(a, mass_shift)
    top = cadd(cadd(g02, cmul(a4, g01)), scale(a_4, g00))
    h01 = scale(top, inv_beta2 / h10)
    low = cadd(cadd(g12, scale(a4, g11)), cmul(a_4, conj(g01)))
    h11 = scale(cadd(low, cmul(conj(a), top)), inv_beta2 / h10_2)
    p = csub(a4, h11)
    q = csub(csub(a_4, scale(h01, h10)), cmul(h11, a))
    left = g22 + size2(p) * g11 + size2(q) * g00
    left = left + 2.0 * (
        cmul(p, conj(g12))[0] + cmul(q, conj(g02))[0] + cmul(cmul(conj(q), p), g01)[0]
    )
    h21_2 = jnp.maximum(left, 0.0) * (inv_beta2 / h10_2) + epsilon
    m00 = size2(h00) + h10_2
    m01 = cadd(cmul(conj(h00), h01), scale(h11, h10))
    m11 = size2(h01) + size2(h11) + h21_2
    t0 = scale(conj(h00), beta)
    t1 = scale(conj(h01), beta)
    inv_l0 = 1.0 / jnp.sqrt(m00)
    l10 = scale(conj(m01), inv_l0)
    f0 = scale(t0, inv_l0)
    inv_d = 1.0 / (m11 - size2(l10))
    y1 = scale(csub(t1, cmul(l10, f0)), inv_d)
    y0 = scale(csub(f0, cmul(conj(l10), y1)), inv_l0)
    inv_beta = 1.0 / beta
    wb = scale(y1, inv_beta / h10)
    wa = cadd(scale(y0, inv_beta), cmul(wb, a))
    return wa, wb


def kernel(
    sizes, b_hbm, l_hbm, sol_ref, res_ref,
    links, edge_links, z_links, rows, field, kv, turned, xbuf, zbuf, zpack, tbuf, tpack, acc, red,
    b_sem, l_sem, sent, got, got_sum, seen_z, seen_x,
):
    nx, nz, nt = sizes
    total_count = nx * nz * nt
    ix, iz, it = lax.axis_index("xy"), lax.axis_index("gz"), lax.axis_index("ta")
    here = (ix * nz + iz) * nt + it
    groups = DOF // 8
    ways = 2 if nx > 2 else 1

    def step(axis_value, by, count):
        return lax.rem(axis_value + (by + count), count)

    def at(x, z, t):
        return (x, z, t)

    line_x = [at(step(ix, d, nx), iz, it) for d in range(1, nx)]
    line_z = [at(ix, step(iz, d, nz), it) for d in range(1, nz)]
    line_t = [at(ix, iz, step(it, d, nt)) for d in range(1, nt)]

    def tell(sem, devices):
        for device in devices:
            pl.semaphore_signal(sem, inc=1, device_id=device, device_id_type=MESH)

    def remote(source, target, send_sem, recv_sem, device):
        return pltpu.make_async_remote_copy(
            src_ref=source, dst_ref=target, send_sem=send_sem, recv_sem=recv_sem,
            device_id=device, device_id_type=MESH,
        )

    b_copy = pltpu.make_async_copy(b_hbm.at[0, 0, 0], field.at[0], b_sem)
    b_copy.start()

    barrier = pltpu.get_barrier_semaphore()
    tell(barrier, line_t + line_z + line_x)

    for number, k, count in ((0, 7, 2), (1, 5, 2), (1, 0, 1), (2, 3, 2), (3, 1, 2)):
        part = pl.ds(k, count)
        pltpu.make_async_copy(l_hbm.at[0, 0, 0, part], links.at[part], l_sem.at[number]).start(priority=1)

    def wait_links(number, count):
        part = links.at[pl.ds(0, count)]
        pltpu.make_async_copy(part, part, l_sem.at[number]).wait()

    lane = lax.broadcasted_iota(jnp.int32, (8, 128), 1)
    row8 = lax.broadcasted_iota(jnp.int32, (8, 128), 0)
    in_t = lane % CT
    in_z = (lane // CT) % CZ
    odd = lane % 2 == 1

    def rolled(x, by):
        return pltpu.roll(x, by % S, 1) if by % S else x

    def seat(j):
        return (in_t == 2 * j) | (in_t == (2 * j + CT - 1) % CT)

    seats = [seat(j) for j in range(groups)]

    def tiles(ref, first, count):
        return [ref[pl.ds(first + 8 * j, 8), :] for j in range(count)]

    def z_rows(h):
        count = groups // 2
        return [(p, h * count + d, (p * count + d) * 8) for p in range(2) for d in range(count)]

    def halo(n):
        mine = kv.at[n]
        for i in range(2 * RHS):
            rows = tiles(mine, i * DOF, groups)
            packed = None
            for j in range(groups):
                part = jnp.where(odd, rolled(rows[j], 2 * j + CT - 1), rolled(rows[j], 2 * j - CT + 1))
                packed = part if packed is None else jnp.where(seats[j], part, packed)
            tpack[n, pl.ds(8 * i, 8), :] = packed
        for way in (0, 1):
            by = 1 if way else -1
            remote(tpack.at[n], tbuf.at[n, way], sent.at[0], got.at[n, 0], at(ix, iz, step(it, by, nt))).start()
        for h in range(2):
            for p, dj, row in z_rows(h):
                a = mine[pl.ds(p * DOF + 8 * dj, 8), :]
                b = mine[pl.ds((2 + p) * DOF + 8 * dj, 8), :]
                zpack[n, h, 0, pl.ds(row, 8), :] = jnp.where(in_z == 0, a, rolled(b, CT))
                zpack[n, h, 1, pl.ds(row, 8), :] = jnp.where(in_z == 0, rolled(a, -CT), b)
            for way in (0, 1):
                by = 1 if way else -1
                remote(
                    zpack.at[n, h, way], zbuf.at[n, h, way], sent.at[0], got.at[n, 2 + h], at(ix, step(iz, by, nz), it)
                ).start()
        for way in range(ways):
            by = 1 if way else -1
            remote(mine, xbuf.at[n, way], sent.at[0], got.at[n, 1], at(step(ix, by, nx), iz, it)).start()

    def receive(n, kind, ref):
        remote(ref, ref, sent.at[0], got.at[n, kind], (ix, iz, it)).wait_recv()

    def products(passes, fresh, merge=False):
        def block(c0):
            sums = [[None] * (3 * RHS) for _ in range(4)]
            for link, near in passes:
                for j in range(groups):
                    rows = pl.ds(8 * j, 8)
                    vs = []
                    for r in range(RHS):
                        vr = near[pl.ds(2 * r * DOF + 8 * j, 8), :]
                        vi = near[pl.ds((2 * r + 1) * DOF + 8 * j, 8), :]
                        vs += [vr, vi, vr + vi]
                    for q in range(4):
                        c = c0 + q
                        lr = links[link, 0, c, rows, :]
                        li = links[link, 1, c, rows, :]
                        if merge:
                            lr = lr + links[link + 1, 0, c, rows, :]
                            li = li + links[link + 1, 1, c, rows, :]
                            links[link, 0, c, rows, :] = lr
                            links[link, 1, c, rows, :] = li
                        ls = (lr, li, lr + li)
                        for m in range(3 * RHS):
                            x = ls[m % 3] * vs[m]
                            sums[q][m] = x if sums[q][m] is None else sums[q][m] + x
            out = []
            for q in range(4):
                parts = []
                for r in range(RHS):
                    rr, ii, both = sums[q][3 * r : 3 * r + 3]
                    parts += [rr - ii, both - (rr + ii)]
                if not fresh:
                    parts = [acc[i, c0 + q] + parts[i] for i in range(2 * RHS)]
                out.append(parts)
            return out

        def body(step_number, carry):
            c0 = step_number * 4
            out = block(c0)
            for q in range(4):
                for i in range(2 * RHS):
                    acc[i, c0 + q] = out[q][i]
            return carry

        lax.fori_loop(0, DOF // 4, body, 0)

    def split_z():
        def body(c, carry):
            for p in range(2):
                for j in range(groups):
                    rows = pl.ds(8 * j, 8)
                    up, down = links[5, p, c, rows, :], links[6, p, c, rows, :]
                    links[5, p, c, rows, :] = jnp.where(in_z == 0, up, down)
                    z_links[p, pl.ds(c * (DOF + 1) + 8 * j, 8), :] = jnp.where(in_z == 0, down, up)
            return carry

        lax.fori_loop(0, DOF, body, 0, unroll=2)

    def pack_edges():
        last = in_t == CT - 1

        def body(c, carry):
            for p in range(2):
                packed = None
                for j in range(groups):
                    rows = pl.ds(8 * j, 8)
                    part = rolled(jnp.where(last, links[7, p, c, rows, :], links[8, p, c, rows, :]), 2 * j)
                    packed = part if packed is None else jnp.where(seats[j], part, packed)
                edge_links[p, pl.ds(pl.multiple_of(8 * c, 8), 8), :] = packed
            return carry

        lax.fori_loop(0, DOF, body, 0, unroll=8)

    low4, low2, low1 = row8 < 4, row8 % 4 < 2, row8 % 2 < 1

    def fold(xs):
        ys = [
            jnp.where(low4, xs[i], xs[i + 4]) + pltpu.roll(jnp.where(low4, xs[i + 4], xs[i]), 4, 0)
            for i in range(4)
        ]
        zs = [
            jnp.where(low2, ys[i] + pltpu.roll(ys[i], 6, 0), ys[i + 2] + pltpu.roll(ys[i + 2], 2, 0))
            for i in range(2)
        ]
        return jnp.where(low1, zs[0] + pltpu.roll(zs[0], 7, 0), zs[1] + pltpu.roll(zs[1], 1, 0))

    def shift(n):
        mine = kv.at[n]
        for j in range(E // 8):
            rows = pl.ds(8 * j, 8)
            own = mine[rows, :]
            turned[0, rows, :] = rolled(own, -CZ * CT)
            turned[1, rows, :] = rolled(own, CZ * CT)
            turned[2, rows, :] = jnp.where(in_z == 0, rolled(own, -CT), rolled(own, CT))
            turned[3, rows, :] = jnp.where(in_t == CT - 1, 0.0, rolled(own, -1))
            turned[4, rows, :] = jnp.where(in_t == 0, 0.0, rolled(own, 1))

    def row_products(link_at, row_at, steps):
        sums = [[None] * groups for _ in range(3 * RHS)]
        for d in steps:
            vs = [jnp.broadcast_to(row_at(m, d), (8, 128)) for m in range(3 * RHS)]
            for g in range(groups):
                lr, li = link_at(0, g, d), link_at(1, g, d)
                ls = (lr, li, lr + li)
                for m in range(3 * RHS):
                    x = ls[m % 3] * vs[m]
                    sums[m][g] = x if sums[m][g] is None else sums[m][g] + x
        out = []
        for r in range(RHS):
            rr, ii, both = sums[3 * r : 3 * r + 3]
            out.append([rr[g] - ii[g] for g in range(groups)])
            out.append([both[g] - (rr[g] + ii[g]) for g in range(groups)])
        return out

    local = ((7, 3), (8, 4), (5, 2), (0, None), (3, 0), (4, 1))

    def near_of(n, terms):
        return [(link, kv.at[n] if near is None else turned.at[near]) for link, near in terms]

    def local_first():
        wait_links(0, 2)
        products(near_of(0, local[:2]), True)
        pack_edges()
        wait_links(1, 3)
        split_z()
        products(near_of(0, local[2:4]), False)

    def apply(n):
        if n == 0:

            @pl.when(it != 0)
            def _():
                shift(0)
                local_first()

            wait_links(2, 2)
            products(near_of(0, local[4:]), False)
            pl.semaphore_wait(seen_z, len(line_z))
            tell(seen_x, line_x)
            wait_links(3, 2)
        else:
            shift(1)
            products(near_of(1, local), True)
            early()
        receive(n, 1, xbuf.at[n, pl.ds(0, ways)])
        if nx > 2:
            products(((1, xbuf.at[n, 0]), (2, xbuf.at[n, 1])), False)
        else:
            products(((1, xbuf.at[n, 0]),), False, n == 0)
        for i in range(4):
            for c in range(0, DOF, 8):
                turned[0, pl.ds(i * DOF + c, 8), :] = fold([acc[i, c + j] for j in range(8)])
        for h in range(2):
            receive(n, 2 + h, zbuf.at[n, h])
            near = {}
            for p, dj, row in z_rows(h):
                p0 = zbuf[n, h, 0, pl.ds(row, 8), :]
                p1 = zbuf[n, h, 1, pl.ds(row, 8), :]
                near[0, p, dj] = jnp.where(in_z == 0, p1, rolled(p0, CT))
                near[1, p, dj] = jnp.where(in_z == 0, rolled(p1, -CT), p0)
            for r, p, dj in near:
                rows[3 * r + p, pl.ds(8 * dj, 8), :] = near[r, p, dj]
                if p == 0:
                    rows[3 * r + 2, pl.ds(8 * dj, 8), :] = near[r, 0, dj] + near[r, 1, dj]
            got_z = row_products(
                lambda p, g, d: z_links[p, pl.ds(8 * g * (DOF + 1) + d, 8, stride=DOF + 1), :],
                lambda m, d: rows[m, pl.ds(d, 1), :],
                range(h * DOF // 2, (h + 1) * DOF // 2),
            )
            for i in range(4):
                for g in range(groups):
                    place = pl.ds(i * DOF + 8 * g, 8)
                    turned[0, place, :] = turned[0, place, :] + got_z[i][g]
        receive(n, 0, tbuf.at[n])
        for r in range(RHS):
            vr, vi = (
                jnp.where(odd, tbuf[n, 0, pl.ds(8 * i, 8), :], tbuf[n, 1, pl.ds(8 * i, 8), :])
                for i in (2 * r, 2 * r + 1)
            )
            for m, v in enumerate((vr, vi, vr + vi)):
                rows[3 * r + m, pl.ds(DOF, 8), :] = v
        got_t = row_products(
            lambda p, g, d: edge_links[p, pl.ds(64 * g + d, 8, stride=8), :],
            lambda m, d: rows[m, pl.ds(DOF + d, 1), :],
            range(8),
        )
        for i in range(4):
            for g in range(groups):
                d = got_t[i][g]
                d = (d + rolled(d, -2)) + (rolled(d, -4) + rolled(d, -6))
                place = pl.ds(i * DOF + 8 * g, 8)
                kv[n + 1, place, :] = turned[0, place, :] + jnp.where(seats[0], d, 0.0)

    def dots(a, b, both):
        out = []
        for r in range(RHS):
            re = im = None
            for j in range(groups):
                ar, ai = (a[pl.ds((2 * r + p) * DOF + 8 * j, 8), :] for p in range(2))
                br, bi = (b[pl.ds((2 * r + p) * DOF + 8 * j, 8), :] for p in range(2))
                x = ar * br + ai * bi
                re = x if re is None else re + x
                if both:
                    x = ar * bi - ai * br
                    im = x if im is None else im + x
            out.append((re, im) if both else (re,))
        return out

    def lane_sums(x):
        return jnp.broadcast_to(jnp.sum(x, axis=1, keepdims=True), (8, 128))

    def early():
        d00, d11, d01 = dots(kv.at[0], kv.at[0], False), dots(kv.at[1], kv.at[1], False), dots(kv.at[0], kv.at[1], True)
        sums = lane_sums(fold([x for r in range(RHS) for x in d00[r] + d11[r] + d01[r]]))
        acc_row = jnp.where(lane == row8, sums, 0.0)
        field[4, pl.ds(0, 8), :] = acc_row

    b_copy.wait()
    kv[0] = field[0].T

    @pl.when(it == 0)
    def _():
        shift(0)
        local_first()

    pl.semaphore_wait(barrier, len(line_t) + len(line_z) + len(line_x))
    halo(0)
    tell(seen_z, line_z)
    apply(0)
    halo(1)
    apply(1)

    d02, d12, d22 = dots(kv.at[0], kv.at[2], True), dots(kv.at[1], kv.at[2], True), dots(kv.at[2], kv.at[2], False)
    sums = lane_sums(fold([x for r in range(RHS) for x in d02[r] + d12[r]]))
    a, b = d22[0][0], d22[1][0]
    norms = lane_sums(jnp.where(low4, a + pltpu.roll(a, 4, 0), b + pltpu.roll(b, 4, 0)))
    mine = field[4, pl.ds(0, 8), :] + jnp.where(lane == 8 + row8, sums, 0.0)
    mine = mine + jnp.where(lane == 16 + row8 // 4, norms, 0.0)
    pl.semaphore_wait(seen_x, len(line_x))
    red[here] = jnp.sum(mine, axis=0, keepdims=True)
    for x, z, t in itertools.product(range(nx), range(nz), range(nt)):

        @pl.when((x * nz + z) * nt + t != here)
        def _():
            remote(red.at[here], red.at[here], sent.at[1], got_sum, (x, z, t)).start()

    in_p = (lax.broadcasted_iota(jnp.int32, (S, E), 1) // DOF) % 2

    def aside(v):
        return jnp.where(in_p == 0, pltpu.roll(v, E - DOF, 1), -pltpu.roll(v, DOF, 1))

    k0, k1, k2 = field[0], kv[1].T, kv[2].T
    low, high = mass_shift * k0 + k1, mass_shift * k1 + k2
    for number, v in enumerate((k0, k1, low, high)):
        if number:
            field[number] = v
        turned[number] = aside(v)
    halo_bytes = links.at[0, 0, pl.ds(0, 2 * (2 + 4 + ways * E // DOF))]
    remote(halo_bytes, halo_bytes, sent.at[0], got_sum, (ix, iz, it)).wait_send()

    others = red.at[pl.ds(0, total_count - 1)]
    remote(others, others, sent.at[1], got_sum, (ix, iz, it)).wait_recv()
    value = jnp.broadcast_to(jnp.sum(red[...], axis=0), (8, 128))
    first_half = lane < 2 * DOF

    def pick(place):
        return [jnp.sum(jnp.where(lane == place + by * r, value, 0.0), axis=1, keepdims=True) for r, by in ((0, 0), (1, 4))]

    place = (row8 // 4) * 8 + row8 % 4
    low, high = pick(place)
    gram = jnp.where(first_half, low, high)
    low, _ = pick(16 + row8 * 0)
    high, _ = pick(17 + row8 * 0)
    g22 = jnp.where(first_half, low, high)[0:1]
    g = [gram[i : i + 1] for i in range(8)]
    wa, wb = coefficients(g[0], g[1], g22, (g[2], g[3]), (g[4], g[5]), (g[6], g[7]))

    wa, wb = ([jnp.broadcast_to(x, (8, 128)) for x in w] for w in (wa, wb))
    for j in range(S // 8):
        rows8 = pl.ds(8 * j, 8)
        k0, k1, low, high = (field[number, rows8, :] for number in range(4))
        z0, z1, z_low, z_high = (turned[number, rows8, :] for number in range(4))
        sol_ref[0, 0, 0, rows8, :] = (wa[0] * k0 - wa[1] * z0) + (wb[0] * k1 - wb[1] * z1)
        res_ref[0, 0, 0, rows8, :] = k0 - (wa[0] * low - wa[1] * z_low) - (wb[0] * high - wb[1] * z_high)
    remote(others, others, sent.at[1], got_sum, (ix, iz, it)).wait_send()


def deliver(a_ref, b_ref, sol_ref, res_ref, sems):
    copies = [pltpu.make_async_copy(a_ref, sol_ref, sems.at[0]), pltpu.make_async_copy(b_ref, res_ref, sems.at[1])]
    for copy in copies:
        copy.start()
    for copy in copies:
        copy.wait()


def shards(sizes, right_side, link_blocks):
    nx, nz, nt = sizes
    out = jax.ShapeDtypeStruct(right_side.shape, jnp.float32)
    f32 = jnp.float32
    held = pltpu.VMEM(right_side.shape, f32)
    results = pl.pallas_call(
        functools.partial(kernel, sizes),
        out_shape=(held, held),
        in_specs=[pl.BlockSpec(memory_space=pl.ANY)] * 2,
        out_specs=(pl.BlockSpec(memory_space=pltpu.VMEM),) * 2,
        scratch_shapes=[
            pltpu.VMEM((9, 2, DOF, DOF, S), f32),
            pltpu.VMEM((2, DOF * 8, S), f32),
            pltpu.VMEM((2, DOF * (DOF + 1), S), f32),
            pltpu.VMEM((3 * RHS, DOF + 8, S), f32),
            pltpu.VMEM((5, S, E), f32),
            pltpu.VMEM((3, E, S), f32),
            pltpu.VMEM((5, E, S), f32),
            pltpu.VMEM((2, 2 if nx > 2 else 1, E, S), f32),
            pltpu.VMEM((2, 2, 2, DOF, S), f32),
            pltpu.VMEM((2, 2, 2, DOF, S), f32),
            pltpu.VMEM((2, 2, 2 * RHS * 8, S), f32),
            pltpu.VMEM((2, 2 * RHS * 8, S), f32),
            pltpu.VMEM((4, DOF, 8, S), f32),
            pltpu.VMEM((nx * nz * nt, 1, 128), f32),
            pltpu.SemaphoreType.DMA,
            pltpu.SemaphoreType.DMA((4,)),
            pltpu.SemaphoreType.DMA((2,)),
            pltpu.SemaphoreType.DMA((2, 4)),
            pltpu.SemaphoreType.DMA,
            pltpu.SemaphoreType.REGULAR,
            pltpu.SemaphoreType.REGULAR,
        ],
        compiler_params=pltpu.CompilerParams(
            collective_id=0, has_side_effects=True, vmem_limit_bytes=56 * 1024 * 1024
        ),
    )(right_side, link_blocks)
    return pl.pallas_call(
        deliver,
        out_shape=(out, out),
        in_specs=[pl.BlockSpec(memory_space=pltpu.VMEM)] * 2,
        out_specs=(pl.BlockSpec(memory_space=pl.ANY),) * 2,
        scratch_shapes=[pltpu.SemaphoreType.DMA((2,))],
    )(*[pltpu.with_memory_space_constraint(x, pltpu.VMEM) for x in results])


def solution(mesh):
    sizes = tuple(mesh.shape[name] for name in ("xy", "gz", "ta"))
    return jax.shard_map(
        functools.partial(shards, sizes),
        mesh=mesh,
        in_specs=(
            P("xy", "gz", "ta", None, None),
            P("xy", "gz", "ta", None, None, None, None, None),
        ),
        out_specs=(P("xy", "gz", "ta", None, None), P("xy", "gz", "ta", None, None)),
        check_vma=False,
    )
```
